16 devices in a mesh: gp: 16 (over z, y, x, core).
Axes of the slice: x: 2, y: 2, z: 2, core: 2. Of those that a mesh axis runs over, the one named last changes fastest.
Arguments:
- grid_in: bfloat16 [16384, 164], P('gp')
- mesh_static: bfloat16 [8192, 3], P('gp')
- edge_static: bfloat16 [24576, 4], P('gp')
- send_rows: int32 [256, 64], P('gp')
- edge_src: int32 [24576], P('gp')
- edge_dst: int32 [24576], P('gp')
- w_grid_in: bfloat16 [164, 256], replicated
- w_mesh_in: bfloat16 [3, 256], replicated
- w_edge_in: bfloat16 [4, 256], replicated
- w_edge_up: bfloat16 [768, 256], replicated
- w_mesh_up: bfloat16 [512, 256], replicated
- w_grid_up: bfloat16 [256, 256], replicated
- w_second: bfloat16 [6, 256, 256], replicated
- vectors: float32 [6, 4, 256], replicated
- d_mesh_out: bfloat16 [8192, 256], P('gp')
- d_grid_out: bfloat16 [16384, 256], P('gp')
Outputs:
- output 1: bfloat16 [8192, 256], P('gp')
- output 2: bfloat16 [16384, 256], P('gp')
- output 3: float32 [16384, 164], P('gp')
- output 4: float32 [164, 256], replicated
- output 5: float32 [3, 256], replicated
- output 6: float32 [4, 256], replicated
- output 7: float32 [768, 256], replicated
- output 8: float32 [512, 256], replicated
- output 9: float32 [256, 256], replicated
- output 10: float32 [6, 256, 256], replicated
- output 11: float32 [6, 4, 256], replicated
All inputs are finite; a program needn't handle non-finite values.
Results may differ from the reference program's by a relative error of at most 0.02.
Values are sent between devices in bfloat16 or wider.
A program may use at most 1 GiB of HBM per device.

```python
import jax
import jax.numpy as jnp
from jax import lax

NUM_PARTS = 16
GRID_DEV = 1024
MESH_DEV = 512
FEATURES = 164
LATENT = 256
MESH_FEAT = 3
EDGE_FEAT = 4
EDGE_DEV = 1536
SLOT_CAP = 64
GRID_ALL = NUM_PARTS * GRID_DEV
MESH_ALL = NUM_PARTS * MESH_DEV
EDGE_ALL = NUM_PARTS * EDGE_DEV
LN_EPS = 1e-5


def draw_indices(key):
    sub_keys = jax.random.split(key, 5)
    band_ids = jnp.arange(NUM_PARTS)
    polar_band = (band_ids == 0) | (band_ids == NUM_PARTS - 1)
    low_cap = SLOT_CAP // 4
    counts = low_cap + jax.random.randint(sub_keys[0], (NUM_PARTS, NUM_PARTS), 0, SLOT_CAP - low_cap + 1, dtype=jnp.int32)
    counts = jnp.where(polar_band[:, None], SLOT_CAP, counts)
    send_rows = jax.random.randint(sub_keys[1], (NUM_PARTS * NUM_PARTS, SLOT_CAP), 0, GRID_DEV, dtype=jnp.int32)
    slot_valid = jnp.arange(SLOT_CAP)[None, None, :] < counts.T[:, :, None]
    buf_len = NUM_PARTS * SLOT_CAP
    slot_valid = slot_valid.reshape(NUM_PARTS, buf_len)
    order_key = jnp.where(slot_valid, 0, buf_len) + jnp.arange(buf_len)[None, :]
    slot_order = jnp.argsort(order_key, axis=1).astype(jnp.int32)
    n_valid = jnp.sum(slot_valid, axis=1).astype(jnp.int32)
    edge_ids = jnp.arange(EDGE_DEV, dtype=jnp.int32)[None, :]
    slot_pick = jax.random.randint(sub_keys[2], (NUM_PARTS, EDGE_DEV), 0, n_valid[:, None], dtype=jnp.int32)
    slot_pick = jnp.where(edge_ids < n_valid[:, None], edge_ids, slot_pick)
    edge_src = jnp.take_along_axis(slot_order, slot_pick, axis=1)
    dst_draw = jax.random.randint(sub_keys[3], (NUM_PARTS, EDGE_DEV), 0, MESH_DEV, dtype=jnp.int32)
    dst_draw = jnp.where(edge_ids < MESH_DEV, edge_ids, dst_draw)
    edge_dst = jax.random.permutation(sub_keys[4], dst_draw, axis=1, independent=True)
    return send_rows, edge_src.reshape(-1).astype(jnp.int32), edge_dst.reshape(-1).astype(jnp.int32)


def weight_draw(key, shape, fan_in):
    return (jax.random.normal(key, shape, jnp.float32) * fan_in ** -0.5).astype(jnp.bfloat16)


def setup_inputs(seed: int = 0) -> dict:
    key = jax.random.key(seed)
    sub_keys = jax.random.split(key, 16)
    send_rows, edge_src, edge_dst = draw_indices(sub_keys[0])
    grid_in = jax.random.normal(sub_keys[1], (GRID_ALL, FEATURES), jnp.float32)
    lat_draw = jax.random.uniform(sub_keys[2], (MESH_ALL,), jnp.float32, -1.5, 1.5)
    lon_draw = jax.random.uniform(sub_keys[3], (MESH_ALL,), jnp.float32, 0.0, 6.28)
    mesh_static = jnp.stack([jnp.cos(lat_draw), jnp.sin(lon_draw), jnp.cos(lon_draw)], axis=1)
    offsets = 0.5 * jax.random.normal(sub_keys[4], (EDGE_ALL, EDGE_FEAT - 1), jnp.float32)
    lengths = jnp.sqrt(jnp.sum(offsets * offsets, axis=1, keepdims=True))
    edge_static = jnp.concatenate([lengths, offsets], axis=1)
    vec_noise = jax.random.normal(sub_keys[12], (6, 4, LATENT), jnp.float32)
    vec_scale = jnp.array([0.3, 0.3, 0.2, 0.3], jnp.float32)
    vec_shift = jnp.array([0.0, 0.0, 1.0, 0.0], jnp.float32)
    vectors = vec_noise * vec_scale[None, :, None] + vec_shift[None, :, None]
    return {
        'grid_in': grid_in.astype(jnp.bfloat16),
        'mesh_static': mesh_static.astype(jnp.bfloat16),
        'edge_static': edge_static.astype(jnp.bfloat16),
        'send_rows': send_rows,
        'edge_src': edge_src,
        'edge_dst': edge_dst,
        'w_grid_in': weight_draw(sub_keys[5], (FEATURES, LATENT), FEATURES),
        'w_mesh_in': weight_draw(sub_keys[6], (MESH_FEAT, LATENT), MESH_FEAT),
        'w_edge_in': weight_draw(sub_keys[7], (EDGE_FEAT, LATENT), EDGE_FEAT),
        'w_edge_up': weight_draw(sub_keys[8], (3 * LATENT, LATENT), 3 * LATENT),
        'w_mesh_up': weight_draw(sub_keys[9], (2 * LATENT, LATENT), 2 * LATENT),
        'w_grid_up': weight_draw(sub_keys[10], (LATENT, LATENT), LATENT),
        'w_second': weight_draw(sub_keys[11], (6, LATENT, LATENT), LATENT),
        'vectors': vectors,
        'd_mesh_out': jax.random.normal(sub_keys[13], (MESH_ALL, LATENT), jnp.float32).astype(jnp.bfloat16),
        'd_grid_out': jax.random.normal(sub_keys[14], (GRID_ALL, LATENT), jnp.float32).astype(jnp.bfloat16),
    }


def mlp_tail(pre_act, w_two, vec_rows):
    pre_bias = pre_act + vec_rows[0]
    hidden = jax.nn.silu(pre_bias).astype(jnp.bfloat16)
    out_lin = jnp.dot(hidden, w_two, preferred_element_type=jnp.float32) + vec_rows[1]
    centered = out_lin - jnp.mean(out_lin, axis=-1, keepdims=True)
    inv_std = lax.rsqrt(jnp.mean(centered * centered, axis=-1, keepdims=True) + LN_EPS)
    return centered * inv_std * vec_rows[2] + vec_rows[3]


def first_layer(feat_in, w_first):
    return jnp.dot(feat_in, w_first, preferred_element_type=jnp.float32)


def reference(grid_in, mesh_static, edge_static, send_rows, edge_src, edge_dst, w_grid_in, w_mesh_in, w_edge_in, w_edge_up, w_mesh_up, w_grid_up, w_second, vectors, d_mesh_out, d_grid_out):
    edge_part = jnp.arange(EDGE_ALL, dtype=jnp.int32) // EDGE_DEV
    band_ids = edge_src // SLOT_CAP
    sender = band_ids * GRID_DEV + send_rows[band_ids * NUM_PARTS + edge_part, edge_src % SLOT_CAP]
    receiver = edge_part * MESH_DEV + edge_dst

    def forward(grid_x, wg_in, wm_in, we_in, we_up, wm_up, wg_up, w_two_all, vec_all):
        grid_lat = mlp_tail(first_layer(grid_x, wg_in), w_two_all[0], vec_all[0]).astype(jnp.bfloat16)
        mesh_lat = mlp_tail(first_layer(mesh_static, wm_in), w_two_all[1], vec_all[1]).astype(jnp.bfloat16)
        edge_lat = mlp_tail(first_layer(edge_static, we_in), w_two_all[2], vec_all[2]).astype(jnp.bfloat16)
        edge_cat = jnp.concatenate([edge_lat, jnp.take(grid_lat, sender, axis=0), jnp.take(mesh_lat, receiver, axis=0)], axis=1)
        edge_new = (edge_lat.astype(jnp.float32) + mlp_tail(first_layer(edge_cat, we_up), w_two_all[3], vec_all[3])).astype(jnp.bfloat16)
        agg_sum = jax.ops.segment_sum(edge_new.astype(jnp.float32), receiver, num_segments=MESH_ALL)
        mesh_cat = jnp.concatenate([mesh_lat, agg_sum.astype(jnp.bfloat16)], axis=1)
        mesh_out = (mesh_lat.astype(jnp.float32) + mlp_tail(first_layer(mesh_cat, wm_up), w_two_all[4], vec_all[4])).astype(jnp.bfloat16)
        grid_out = (grid_lat.astype(jnp.float32) + mlp_tail(first_layer(grid_lat, wg_up), w_two_all[5], vec_all[5])).astype(jnp.bfloat16)
        return mesh_out, grid_out

    fwd_outs, pull_back = jax.vjp(forward, grid_in, w_grid_in, w_mesh_in, w_edge_in, w_edge_up, w_mesh_up, w_grid_up, w_second, vectors)
    all_grads = pull_back((d_mesh_out, d_grid_out))
    return (fwd_outs[0], fwd_outs[1], all_grads[0].astype(jnp.float32), all_grads[1].astype(jnp.float32), all_grads[2].astype(jnp.float32), all_grads[3].astype(jnp.float32), all_grads[4].astype(jnp.float32), all_grads[5].astype(jnp.float32), all_grads[6].astype(jnp.float32), all_grads[7].astype(jnp.float32), all_grads[8].astype(jnp.float32))
```

```python
import functools

import jax
import jax.numpy as jnp
from jax import lax
from jax.experimental import pallas as pl
from jax.experimental.pallas import tpu as pltpu
from jax.sharding import PartitionSpec as P

LN_EPS = 1e-5
AXIS_NAME = 'gp'
N_DEV = 16
N_CHIP = 8
LAT = 256
BLK = 256
F32 = jnp.float32
BF16 = jnp.bfloat16

GROUP_ROWS = (512, 1792, 512, 512)
ROW_EDGE_IN = 168
ROW_MESH_IN = 176
ROW_VEC = 184


def mm(a, b):
    return lax.dot_general(a, b, (((1,), (0,)), ((), ())), preferred_element_type=F32)


def mm_nt(a, b):
    return lax.dot_general(a, b, (((1,), (1,)), ((), ())), preferred_element_type=F32)


def mm_tn(a, b):
    return lax.dot_general(a, b, (((0,), (0,)), ((), ())), preferred_element_type=F32)


def fold8(x):
    return jnp.sum(x.reshape(-1, 8, x.shape[-1]), axis=0)


def main_kernel(
        grid_in, mesh_static, edge_static, send_rows, edge_src, edge_dst,
        w_grid_in, w_mesh_in, w_edge_in, w_edge_up, w_mesh_up, w_grid_up, w_second, vectors, d_mesh_out, d_grid_out,
        mesh_out, grid_out, d_grid_in, res0, res1, res2, res3,
        grid_lat, mesh_lat, edge_lat, outgoing, incoming, d_incoming, d_outgoing,
        oh_src, oht_src, oh_dst, oht_dst,
        hid0, hid1, hid2, hid3, hid4, hid5,
        ds0, ds1, ds2, ds3, nm0, nm1, nm2, nm3, iv0, iv1, iv2, iv3,
        part3, edge_new, agg, d_grid_lat, d_mesh_lat, d_edge_lat, d_agg, d_slot, d_node,
        dl_g, dp_g, dl_m4, dp_m4, dl_e3, dp_e3, dl_e2, dp_e2, dl_m1, dp_m1, dl_g0, dp_g0,
        par0, par1, par2, par3, ra0, ra1, ra2, ra3, cs0, cs1, cs2, cs3, rb0, rb1, rb2, rb3,
        f_send, f_recv, b_send, b_recv, s0_send, s0_recv, s1_send, s1_recv, s2_send, s2_recv, s3_send, s3_recv):
    me = lax.axis_index(AXIS_NAME)
    core = me % 2
    chip = me // 2
    n_grid = grid_lat.shape[0]
    n_mesh = mesh_lat.shape[0]
    n_edge = edge_lat.shape[0]
    slots = send_rows.shape[1]
    pars, ras, css, rbs, ress = (par0, par1, par2, par3), (ra0, ra1, ra2, ra3), (cs0, cs1, cs2, cs3), (rb0, rb1, rb2, rb3), (res0, res1, res2, res3)

    def flip(idx, j):
        out = 0
        for b in range(4):
            bit = (idx // (1 << b)) % 2
            out = out + (1 << b) * (1 - bit if (j >> b) & 1 else bit)
        return out

    barrier = pltpu.get_barrier_semaphore()
    for j in range(1, N_DEV):
        pl.semaphore_signal(barrier, inc=1, device_id=(flip(me, j),), device_id_type=pl.DeviceIdType.MESH)

    pending = []

    def send(src, dst, send_sem, recv_sem, dev):
        copy = pltpu.make_async_remote_copy(src_ref=src, dst_ref=dst, send_sem=send_sem, recv_sem=recv_sem,
                                            device_id=(dev,), device_id_type=pl.DeviceIdType.MESH)
        copy.start()
        pending.append(copy)
        return copy

    far_first = (15, 14, 7, 6, 11, 10, 13, 12, 3, 2, 5, 4, 9, 8, 1)
    chip_order = (7, 3, 5, 6, 1, 2, 4)

    def exchange(src, dst, send_sem, recv_sem):
        copies = []
        for j in far_first:
            peer = flip(me, j)
            copies.append(send(src.at[pl.ds(pl.multiple_of(peer * slots, slots), slots)],
                               dst.at[pl.ds(pl.multiple_of(me * slots, slots), slots)],
                               send_sem.at[j], recv_sem.at[j], peer))
        mine = pl.ds(pl.multiple_of(me * slots, slots), slots)
        dst[mine, :] = src[mine, :]
        return copies

    live = {}

    def stage0(g):
        half = GROUP_ROWS[g] // 2
        other = pl.ds(pl.multiple_of((1 - core) * half, half), half)
        live[g] = [send(pars[g].at[other], ras[g], s0_send.at[g], s0_recv.at[g], flip(me, 1))]

    def stage1(g):
        live[g][0].wait_recv()
        half = GROUP_ROWS[g] // 2
        part = half // N_CHIP
        mine = pl.ds(pl.multiple_of(core * half, half), half)
        total = pars[g][mine, :] + ras[g][...]
        ras[g][...] = total
        css[g][...] = total.astype(BF16)
        copies = []
        for j in chip_order:
            peer = flip(me, 2 * j)
            copies.append(send(css[g].at[pl.ds(pl.multiple_of((peer // 2) * part, part), part)], rbs[g].at[j - 1],
                               s1_send.at[g, j], s1_recv.at[g, j], peer))
        live[g] = copies

    def stage2(g):
        half = GROUP_ROWS[g] // 2
        part = half // N_CHIP
        for copy in live[g]:
            copy.wait_recv()
        total = ras[g][pl.ds(pl.multiple_of(chip * part, part), part), :]
        for j in range(1, N_CHIP):
            total = total + rbs[g][j - 1].astype(F32)
        mine = pl.ds(pl.multiple_of(core * half + chip * part, part), part)
        ress[g][mine, :] = total.astype(BF16)
        copies = []
        for j in chip_order:
            copies.append(send(ress[g].at[mine], ress[g].at[mine], s2_send.at[g, j], s2_recv.at[g, j], flip(me, 2 * j)))
        live[g] = copies

    def stage3(g):
        half = GROUP_ROWS[g] // 2
        for copy in live[g]:
            copy.wait_recv()
        mine = pl.ds(pl.multiple_of(core * half, half), half)
        live[g] = [send(ress[g].at[mine], ress[g].at[mine], s3_send.at[g], s3_recv.at[g], flip(me, 1))]

    def stage4(g):
        live[g][0].wait_recv()

    def blk(i, size=BLK):
        return pl.ds(pl.multiple_of(i * size, size), size)

    def vec(k, i):
        return vectors[k, i:i + 1, :]

    def mlp_fwd(k, pre):
        x = pre + vec(k, 0)
        sig = jax.nn.sigmoid(x)
        act = x * sig
        hid = act.astype(BF16)
        o = mm(hid, w_second[k]) + vec(k, 1)
        cen = o - jnp.mean(o, axis=-1, keepdims=True)
        inv = lax.rsqrt(jnp.mean(cen * cen, axis=-1, keepdims=True) + LN_EPS)
        nrm = cen * inv
        out = nrm * vec(k, 2) + vec(k, 3)
        dsilu = sig + act * (1.0 - sig)
        return out, hid, dsilu, nrm, inv

    def mlp_bwd(k, dsilu, nrm, inv, d_out):
        dn = d_out * vec(k, 2)
        m1 = jnp.mean(dn, axis=-1, keepdims=True)
        m2 = jnp.mean(dn * nrm, axis=-1, keepdims=True)
        d_lin = inv * (dn - m1 - nrm * m2)
        d_lin_bf = d_lin.astype(BF16)
        d_pre = mm_nt(d_lin_bf, w_second[k]) * dsilu
        return d_lin_bf, d_pre.astype(BF16), (fold8(d_pre), fold8(d_lin), fold8(d_out * nrm), fold8(d_out))

    zeros4 = tuple(jnp.zeros((8, LAT), F32) for _ in range(4))

    def put_vec(k, sums):
        for i in range(4):
            par3[256 + ROW_VEC + 4 * k + i:256 + ROW_VEC + 4 * k + i + 1, :] = jnp.sum(sums[i], axis=0, keepdims=True)

    def add4(a, b):
        return tuple(x + y for x, y in zip(a, b))

    par3[256:512, :] = jnp.zeros((256, LAT), F32)

    def grid_embed(i, c):
        rows = blk(i)
        out, hid, dsilu, nrm, inv = mlp_fwd(0, mm(grid_in[rows, :], w_grid_in[...]))
        grid_lat[rows, :] = out.astype(BF16)
        hid0[rows, :] = hid
        ds0[rows, :] = dsilu
        nm0[rows, :] = nrm
        iv0[rows, :] = inv
        return c

    lax.fori_loop(0, n_grid // BLK, grid_embed, 0)

    def row_pair(i):
        return jnp.concatenate([send_rows[2 * i:2 * i + 1, :], send_rows[2 * i + 1:2 * i + 2, :]], axis=1)

    def columns_of(row):
        return jnp.transpose(jnp.broadcast_to(row, (128, 128)))

    def one_hot(col, n):
        lane = lax.broadcasted_iota(jnp.int32, (128, 128), 1)
        return jnp.concatenate([jnp.where(col - 128 * t == lane, 1.0, 0.0).astype(BF16) for t in range(n // 128)], axis=1)

    def one_hot_t(row, n):
        sub = lax.broadcasted_iota(jnp.int32, (n, 128), 0)
        return jnp.where(sub == row, 1.0, 0.0).astype(BF16)

    for i in range(N_DEV // 2):
        pick = one_hot(columns_of(row_pair(i)), n_grid)
        outgoing[128 * i:128 * (i + 1), :] = mm(pick, grid_lat[...]).astype(BF16)

    pl.semaphore_wait(barrier, N_DEV - 1)
    fwd = exchange(outgoing, incoming, f_send, f_recv)

    def grid_update(i, sums):
        rows = blk(i)
        lat = grid_lat[rows, :]
        out, hid, dsilu, nrm, inv = mlp_fwd(5, mm(lat, w_grid_up[...]))
        grid_out[rows, :] = (lat.astype(F32) + out).astype(BF16)
        d_out = d_grid_out[rows, :].astype(F32)
        d_lin, d_pre, add = mlp_bwd(5, dsilu, nrm, inv, d_out)
        hid5[rows, :] = hid
        dl_g[rows, :] = d_lin
        dp_g[rows, :] = d_pre
        d_grid_lat[rows, :] = d_out + mm_nt(d_pre, w_grid_up[...])
        return add4(sums, add)

    put_vec(5, lax.fori_loop(0, n_grid // BLK, grid_update, zeros4))
    par0[0:256, :] = mm_tn(grid_lat[...], dp_g[...])
    par0[256:512, :] = mm_tn(hid5[...], dl_g[...])
    stage0(0)

    def mesh_embed(i, c):
        rows = blk(i)
        out, hid, dsilu, nrm, inv = mlp_fwd(1, mm(mesh_static[rows, :], w_mesh_in[...]))
        mesh_lat[rows, :] = out.astype(BF16)
        hid1[rows, :] = hid
        ds1[rows, :] = dsilu
        nm1[rows, :] = nrm
        iv1[rows, :] = inv
        return c

    lax.fori_loop(0, n_mesh // BLK, mesh_embed, 0)

    def hots(i, c):
        rows = blk(i, 128)
        src = edge_src[pl.ds(i, 1), :]
        dst = edge_dst[pl.ds(i, 1), :]
        oh_src[rows, :] = one_hot(columns_of(src), n_grid)
        oh_dst[rows, :] = one_hot(columns_of(dst), n_mesh)
        oht_src[:, rows] = one_hot_t(src, n_grid)
        oht_dst[:, rows] = one_hot_t(dst, n_mesh)
        return c

    lax.fori_loop(0, n_edge // 128, hots, 0)
    stage1(0)

    def edge_embed(i, c):
        rows = blk(i)
        out, hid, dsilu, nrm, inv = mlp_fwd(2, mm(edge_static[rows, :], w_edge_in[...]))
        lat = out.astype(BF16)
        edge_lat[rows, :] = lat
        hid2[rows, :] = hid
        ds2[rows, :] = dsilu
        nm2[rows, :] = nrm
        iv2[rows, :] = inv
        recv = mm(oh_dst[rows, :], mesh_lat[...]).astype(BF16)
        part3[rows, :] = mm(lat, w_edge_up[0:LAT, :]) + mm(recv, w_edge_up[2 * LAT:3 * LAT, :])
        return c

    lax.fori_loop(0, n_edge // BLK, edge_embed, 0)
    stage2(0)

    for copy in fwd:
        copy.wait_recv()

    def edge_update(i, c):
        rows = blk(i)
        sender = mm(oh_src[rows, :], incoming[...]).astype(BF16)
        out, hid, dsilu, nrm, inv = mlp_fwd(3, part3[rows, :] + mm(sender, w_edge_up[LAT:2 * LAT, :]))
        edge_new[rows, :] = (edge_lat[rows, :].astype(F32) + out).astype(BF16)
        hid3[rows, :] = hid
        ds3[rows, :] = dsilu
        nm3[rows, :] = nrm
        iv3[rows, :] = inv
        return c

    lax.fori_loop(0, n_edge // BLK, edge_update, 0)
    stage3(0)

    def mesh_update(i, sums):
        rows = blk(i)
        total = mm(oht_dst[rows, :], edge_new[...]).astype(BF16)
        agg[rows, :] = total
        lat = mesh_lat[rows, :]
        out, hid, dsilu, nrm, inv = mlp_fwd(4, mm(lat, w_mesh_up[0:LAT, :]) + mm(total, w_mesh_up[LAT:2 * LAT, :]))
        mesh_out[rows, :] = (lat.astype(F32) + out).astype(BF16)
        d_out = d_mesh_out[rows, :].astype(F32)
        d_lin, d_pre, add = mlp_bwd(4, dsilu, nrm, inv, d_out)
        hid4[rows, :] = hid
        dl_m4[rows, :] = d_lin
        dp_m4[rows, :] = d_pre
        d_mesh_lat[rows, :] = d_out + mm_nt(d_pre, w_mesh_up[0:LAT, :])
        d_agg[rows, :] = mm_nt(d_pre, w_mesh_up[LAT:2 * LAT, :]).astype(BF16)
        return add4(sums, add)

    put_vec(4, lax.fori_loop(0, n_mesh // BLK, mesh_update, zeros4))

    def edge_back(i, sums):
        rows = blk(i)
        d_out = mm(oh_dst[rows, :], d_agg[...])
        d_lin, d_pre, add = mlp_bwd(3, ds3[rows, :], nm3[rows, :], iv3[rows, :], d_out)
        dl_e3[rows, :] = d_lin
        dp_e3[rows, :] = d_pre
        d_edge_lat[rows, :] = d_out + mm_nt(d_pre, w_edge_up[0:LAT, :])
        return add4(sums, add)

    put_vec(3, lax.fori_loop(0, n_edge // BLK, edge_back, zeros4))

    def slot_back(i, c):
        rows = blk(i)
        d_sum = mm(oht_src[rows, :], dp_e3[...]).astype(BF16)
        d_slot[rows, :] = d_sum
        d_incoming[rows, :] = mm_nt(d_sum, w_edge_up[LAT:2 * LAT, :]).astype(BF16)
        return c

    lax.fori_loop(0, n_grid // BLK, slot_back, 0)
    bwd = exchange(d_incoming, d_outgoing, b_send, b_recv)

    def node_back(i, c):
        rows = blk(i)
        d_sum = mm(oht_dst[rows, :], dp_e3[...]).astype(BF16)
        d_node[rows, :] = d_sum
        d_mesh_lat[rows, :] = d_mesh_lat[rows, :] + mm_nt(d_sum, w_edge_up[2 * LAT:3 * LAT, :])
        return c

    lax.fori_loop(0, n_mesh // BLK, node_back, 0)
    par1[0:256, :] = mm_tn(edge_lat[...], dp_e3[...])
    par1[256:512, :] = mm_tn(incoming[...], d_slot[...])
    par1[512:768, :] = mm_tn(mesh_lat[...], d_node[...])
    par1[768:1024, :] = mm_tn(hid3[...], dl_e3[...])
    par1[1024:1280, :] = mm_tn(mesh_lat[...], dp_m4[...])
    par1[1280:1536, :] = mm_tn(agg[...], dp_m4[...])
    par1[1536:1792, :] = mm_tn(hid4[...], dl_m4[...])
    stage0(1)

    def mesh_in_back(i, sums):
        rows = blk(i)
        d_lin, d_pre, add = mlp_bwd(1, ds1[rows, :], nm1[rows, :], iv1[rows, :], d_mesh_lat[rows, :])
        dl_m1[rows, :] = d_lin
        dp_m1[rows, :] = d_pre
        return add4(sums, add)

    put_vec(1, lax.fori_loop(0, n_mesh // BLK, mesh_in_back, zeros4))
    stage1(1)

    def edge_in_back(i, sums):
        rows = blk(i)
        d_lin, d_pre, add = mlp_bwd(2, ds2[rows, :], nm2[rows, :], iv2[rows, :], d_edge_lat[rows, :])
        dl_e2[rows, :] = d_lin
        dp_e2[rows, :] = d_pre
        return add4(sums, add)

    put_vec(2, lax.fori_loop(0, n_edge // BLK, edge_in_back, zeros4))
    par2[0:256, :] = mm_tn(hid2[...], dl_e2[...])
    par2[256:512, :] = mm_tn(hid1[...], dl_m1[...])
    stage0(2)
    par3[256 + ROW_EDGE_IN:256 + ROW_EDGE_IN + 4, :] = mm_tn(edge_static[...], dp_e2[...])
    par3[256 + ROW_MESH_IN:256 + ROW_MESH_IN + 3, :] = mm_tn(mesh_static[...], dp_m1[...])
    stage2(1)

    for copy in bwd:
        copy.wait_recv()

    all_rows = jnp.concatenate([row_pair(i) for i in range(N_DEV // 2)], axis=1)

    def grid_in_back(i, sums):
        rows = blk(i)
        sub = lax.broadcasted_iota(jnp.int32, (BLK, N_DEV * slots), 0) + i * BLK
        spread = jnp.where(sub == all_rows, 1.0, 0.0).astype(BF16)
        d_out = d_grid_lat[rows, :] + mm(spread, d_outgoing[...])
        d_lin, d_pre, add = mlp_bwd(0, ds0[rows, :], nm0[rows, :], iv0[rows, :], d_out)
        dl_g0[rows, :] = d_lin
        dp_g0[rows, :] = d_pre
        d_grid_in[rows, :] = mm_nt(d_pre, w_grid_in[...])
        return add4(sums, add)

    put_vec(0, lax.fori_loop(0, n_grid // BLK, grid_in_back, zeros4))
    par3[0:256, :] = mm_tn(hid0[...], dl_g0[...])
    par3[256:256 + grid_in.shape[1], :] = mm_tn(grid_in[...], dp_g0[...])
    stage0(3)
    stage1(2)
    stage3(1)
    stage1(3)
    stage2(2)
    stage2(3)
    stage3(2)
    stage3(3)
    for g in range(4):
        stage4(g)
    for copy in pending:
        copy.wait_send()


def final_kernel(mesh_res, grid_res, d_grid_res, res0, res1, res2, res3,
                 mesh_out, grid_out, d_grid_in, d_w_grid_in, d_w_mesh_in, d_w_edge_in, d_w_edge_up, d_w_mesh_up, d_w_grid_up, d_w_second, d_vectors):
    mesh_out[...] = mesh_res[...]
    grid_out[...] = grid_res[...]
    d_grid_in[...] = d_grid_res[...]
    d_w_grid_up[...] = res0[0:256, :].astype(F32)
    d_w_second[5] = res0[256:512, :].astype(F32)
    d_w_edge_up[...] = res1[0:768, :].astype(F32)
    d_w_second[3] = res1[768:1024, :].astype(F32)
    d_w_mesh_up[...] = res1[1024:1536, :].astype(F32)
    d_w_second[4] = res1[1536:1792, :].astype(F32)
    d_w_second[2] = res2[0:256, :].astype(F32)
    d_w_second[1] = res2[256:512, :].astype(F32)
    d_w_second[0] = res3[0:256, :].astype(F32)
    small = res3[256:512, :].astype(F32)
    d_w_grid_in[...] = small[0:d_w_grid_in.shape[0], :]
    d_w_edge_in[...] = small[ROW_EDGE_IN:ROW_EDGE_IN + 4, :]
    d_w_mesh_in[...] = small[ROW_MESH_IN:ROW_MESH_IN + 3, :]
    d_vectors[...] = small[ROW_VEC:ROW_VEC + 24, :].reshape(6, 4, LAT)


def solution(mesh):
    row_spec = P(AXIS_NAME, None)
    edge_spec = P(AXIS_NAME)
    rep_spec = P()
    in_specs = (row_spec, row_spec, row_spec, row_spec, edge_spec, edge_spec) + (rep_spec,) * 8 + (row_spec, row_spec)
    out_specs = (row_spec, row_spec, row_spec) + (rep_spec,) * 8

    def local_step(grid_in, mesh_static, edge_static, send_rows, edge_src, edge_dst, *rest):
        n_grid, feats = grid_in.shape
        n_mesh = mesh_static.shape[0]
        n_edge = edge_static.shape[0]
        n_slot = send_rows.size
        src2 = edge_src.reshape(n_edge // 128, 128)
        dst2 = edge_dst.reshape(n_edge // 128, 128)

        def vm(shape, dtype):
            return pltpu.VMEM(shape, dtype)

        def rows_bf(n):
            return vm((n, LAT), BF16)

        def rows_f32(n):
            return vm((n, LAT), F32)

        dma = pltpu.SemaphoreType.DMA
        scratch = [
            rows_bf(n_grid), rows_bf(n_mesh), rows_bf(n_edge), rows_bf(n_slot), rows_bf(n_slot), rows_bf(n_slot), rows_bf(n_slot),
            vm((n_edge, n_slot), BF16), vm((n_slot, n_edge), BF16), vm((n_edge, n_mesh), BF16), vm((n_mesh, n_edge), BF16),
            rows_bf(n_grid), rows_bf(n_mesh), rows_bf(n_edge), rows_bf(n_edge), rows_bf(n_mesh), rows_bf(n_grid),
            rows_f32(n_grid), rows_f32(n_mesh), rows_f32(n_edge), rows_f32(n_edge),
            rows_f32(n_grid), rows_f32(n_mesh), rows_f32(n_edge), rows_f32(n_edge),
            vm((n_grid, 1), F32), vm((n_mesh, 1), F32), vm((n_edge, 1), F32), vm((n_edge, 1), F32),
            rows_f32(n_edge), rows_bf(n_edge), rows_bf(n_mesh), rows_f32(n_grid), rows_f32(n_mesh), rows_f32(n_edge), rows_bf(n_mesh), rows_bf(n_slot), rows_bf(n_mesh),
            rows_bf(n_grid), rows_bf(n_grid), rows_bf(n_mesh), rows_bf(n_mesh), rows_bf(n_edge), rows_bf(n_edge), rows_bf(n_edge), rows_bf(n_edge), rows_bf(n_mesh), rows_bf(n_mesh), rows_bf(n_grid), rows_bf(n_grid),
        ]
        scratch += [rows_f32(r) for r in GROUP_ROWS]
        scratch += [rows_f32(r // 2) for r in GROUP_ROWS]
        scratch += [rows_bf(r // 2) for r in GROUP_ROWS]
        scratch += [vm((7, r // 16, LAT), BF16) for r in GROUP_ROWS]
        scratch += [dma((16,)), dma((16,)), dma((16,)), dma((16,)), dma((4,)), dma((4,)), dma((4, 8)), dma((4, 8)), dma((4, 8)), dma((4, 8)), dma((4,)), dma((4,))]
        shape = jax.ShapeDtypeStruct
        outs = (shape((n_mesh, LAT), BF16), shape((n_grid, LAT), BF16), shape((n_grid, feats), F32)) + tuple(shape((r, LAT), BF16) for r in GROUP_ROWS)
        vspec = pl.BlockSpec(memory_space=pltpu.VMEM)
        results = pl.pallas_call(
            main_kernel,
            out_shape=outs,
            in_specs=[vspec] * 16,
            out_specs=tuple([vspec] * len(outs)),
            scratch_shapes=scratch,
            compiler_params=pltpu.CompilerParams(collective_id=0, has_side_effects=True, vmem_limit_bytes=63 * 1024 * 1024),
        )(grid_in, mesh_static, edge_static, send_rows, src2, dst2, *rest)

        finals = (shape((n_mesh, LAT), BF16), shape((n_grid, LAT), BF16), shape((n_grid, feats), F32),
                  shape((feats, LAT), F32), shape((3, LAT), F32), shape((4, LAT), F32), shape((3 * LAT, LAT), F32),
                  shape((2 * LAT, LAT), F32), shape((LAT, LAT), F32), shape((6, LAT, LAT), F32), shape((6, 4, LAT), F32))
        return pl.pallas_call(
            final_kernel,
            out_shape=finals,
            in_specs=[vspec] * len(outs),
            out_specs=tuple([vspec] * len(finals)),
        )(*results)

    return jax.shard_map(local_step, mesh=mesh, in_specs=in_specs, out_specs=out_specs, check_vma=False)
```

```python
import functools

import jax
import jax.numpy as jnp
from jax import lax
from jax.experimental import pallas as pl
from jax.experimental.pallas import tpu as pltpu
from jax.sharding import PartitionSpec as P

LN_EPS = 1e-5
AXIS_NAME = 'gp'
N_DEV = 16
N_CHIP = 8
LAT = 256
BLK_G, BLK_M, BLK_E, BLK_S = 1024, 512, 768, 1024
F32 = jnp.float32
BF16 = jnp.bfloat16

GROUP_ROWS = (512, 768, 1024, 512, 512)
N_GROUP = len(GROUP_ROWS)
ROW_EDGE_IN = 168
ROW_MESH_IN = 176
ROW_VEC = 184


def mm(a, b):
    return lax.dot_general(a, b, (((1,), (0,)), ((), ())), preferred_element_type=F32)


def mm_nt(a, b):
    return lax.dot_general(a, b, (((1,), (1,)), ((), ())), preferred_element_type=F32)


def mm_tn(a, b):
    return lax.dot_general(a, b, (((0,), (0,)), ((), ())), preferred_element_type=F32)


def fold8(x):
    return jnp.sum(x.reshape(-1, 8, x.shape[-1]), axis=0)


def main_kernel(
        grid_in, mesh_static, edge_static, send_rows, edge_src, edge_dst,
        w_grid_in, w_mesh_in, w_edge_in, w_edge_up, w_mesh_up, w_grid_up, w_second, vectors, d_mesh_out, d_grid_out,
        mesh_out, grid_out, d_grid_in, res0, res1, res2, res3, res4,
        grid_lat, mesh_lat, edge_lat, outgoing, incoming, d_incoming, d_outgoing,
        oh_src, oht_src, oh_dst, oht_dst,
        hid0, hid1, hid2, hid3, hid4, hid5,
        ds0, ds1, ds2, ds3, nm0, nm1, nm2, nm3, iv0, iv1, iv2, iv3,
        part3, edge_new, agg, d_grid_lat, d_mesh_lat, d_agg, d_slot, d_node,
        dl_g, dp_g, dl_m, dp_m, dl_e, dp_e,
        par0, par1, par2, par3, par4, ra0, ra1, ra2, ra3, ra4, cs0, cs1, cs2, cs3, cs4, rb0, rb1, rb2, rb3, rb4,
        f_send, f_recv, b_send, b_recv, s0_send, s0_recv, s1_send, s1_recv, s2_send, s2_recv, s3_send, s3_recv):
    me = lax.axis_index(AXIS_NAME)
    core = me % 2
    chip = me // 2
    n_grid = grid_lat.shape[0]
    n_mesh = mesh_lat.shape[0]
    n_edge = edge_lat.shape[0]
    slots = send_rows.shape[1]
    pars, ras, css = (par0, par1, par2, par3, par4), (ra0, ra1, ra2, ra3, ra4), (cs0, cs1, cs2, cs3, cs4)
    rbs, ress = (rb0, rb1, rb2, rb3, rb4), (res0, res1, res2, res3, res4)

    def flip(idx, j):
        out = 0
        for b in range(4):
            bit = (idx // (1 << b)) % 2
            out = out + (1 << b) * (1 - bit if (j >> b) & 1 else bit)
        return out

    def loop(name, lo, hi, body, init):
        with jax.named_scope(name):
            return lax.fori_loop(lo, hi, body, init)

    barrier = pltpu.get_barrier_semaphore()
    for j in range(1, N_DEV):
        pl.semaphore_signal(barrier, inc=1, device_id=(flip(me, j),), device_id_type=pl.DeviceIdType.MESH)

    pending = []

    def send(src, dst, send_sem, recv_sem, dev):
        copy = pltpu.make_async_remote_copy(src_ref=src, dst_ref=dst, send_sem=send_sem, recv_sem=recv_sem,
                                            device_id=(dev,), device_id_type=pl.DeviceIdType.MESH)
        copy.start()
        pending.append(copy)
        return copy

    far_first = (15, 14, 7, 6, 11, 10, 13, 12, 3, 2, 5, 4, 9, 8, 1)
    chip_order = (7, 3, 5, 6, 1, 2, 4)

    def exchange(src, dst, send_sem, recv_sem):
        copies = []
        for j in far_first:
            peer = flip(me, j)
            copies.append(send(src.at[pl.ds(pl.multiple_of(peer * slots, slots), slots)],
                               dst.at[pl.ds(pl.multiple_of(me * slots, slots), slots)],
                               send_sem.at[j], recv_sem.at[j], peer))
        mine = pl.ds(pl.multiple_of(me * slots, slots), slots)
        dst[mine, :] = src[mine, :]
        return copies

    live = {}

    def stage0(g):
        half = GROUP_ROWS[g] // 2
        other = pl.ds(pl.multiple_of((1 - core) * half, half), half)
        live[g] = [send(pars[g].at[other], ras[g], s0_send.at[g], s0_recv.at[g], flip(me, 1))]

    def stage1(g):
        with jax.named_scope('s1_%d' % g):
            live[g][0].wait_recv()
            half = GROUP_ROWS[g] // 2
            part = half // N_CHIP
            mine = pl.ds(pl.multiple_of(core * half, half), half)
            total = pars[g][mine, :] + ras[g][...]
            ras[g][...] = total
            css[g][...] = total.astype(BF16)
            copies = []
            for j in chip_order:
                peer = flip(me, 2 * j)
                copies.append(send(css[g].at[pl.ds(pl.multiple_of((peer // 2) * part, part), part)], rbs[g].at[j - 1],
                                   s1_send.at[g, j], s1_recv.at[g, j], peer))
            live[g] = copies

    def stage2(g):
        with jax.named_scope('s2_%d' % g):
            half = GROUP_ROWS[g] // 2
            part = half // N_CHIP
            for copy in live[g]:
                copy.wait_recv()
            total = ras[g][pl.ds(pl.multiple_of(chip * part, part), part), :]
            for j in range(1, N_CHIP):
                total = total + rbs[g][j - 1].astype(F32)
            mine = pl.ds(pl.multiple_of(core * half + chip * part, part), part)
            ress[g][mine, :] = total.astype(BF16)
            copies = []
            for j in chip_order:
                copies.append(send(ress[g].at[mine], ress[g].at[mine], s2_send.at[g, j], s2_recv.at[g, j], flip(me, 2 * j)))
            live[g] = copies

    def stage3(g):
        with jax.named_scope('s3_%d' % g):
            half = GROUP_ROWS[g] // 2
            for copy in live[g]:
                copy.wait_recv()
            mine = pl.ds(pl.multiple_of(core * half, half), half)
            live[g] = [send(ress[g].at[mine], ress[g].at[mine], s3_send.at[g], s3_recv.at[g], flip(me, 1))]

    def stage4(g):
        with jax.named_scope('s4_%d' % g):
            live[g][0].wait_recv()

    def blk(i, size):
        return pl.ds(pl.multiple_of(i * size, size), size)

    def vec(k, i):
        return vectors[k, i:i + 1, :]

    def mlp_fwd(k, pre):
        x = pre + vec(k, 0)
        sig = jax.nn.sigmoid(x)
        act = x * sig
        hid = act.astype(BF16)
        o = mm(hid, w_second[k]) + vec(k, 1)
        cen = o - jnp.mean(o, axis=-1, keepdims=True)
        inv = lax.rsqrt(jnp.mean(cen * cen, axis=-1, keepdims=True) + LN_EPS)
        nrm = cen * inv
        out = nrm * vec(k, 2) + vec(k, 3)
        dsilu = sig + act * (1.0 - sig)
        return out, hid, dsilu, nrm, inv

    def mlp_bwd(k, dsilu, nrm, inv, d_out):
        dn = d_out * vec(k, 2)
        m1 = jnp.mean(dn, axis=-1, keepdims=True)
        m2 = jnp.mean(dn * nrm, axis=-1, keepdims=True)
        d_lin = inv * (dn - m1 - nrm * m2)
        d_lin_bf = d_lin.astype(BF16)
        d_pre = mm_nt(d_lin_bf, w_second[k]) * dsilu
        return d_lin_bf, d_pre.astype(BF16), (fold8(d_pre), fold8(d_lin), fold8(d_out * nrm), fold8(d_out))

    zeros4 = tuple(jnp.zeros((8, LAT), F32) for _ in range(4))

    def put_vec(k, sums):
        for i in range(4):
            par4[256 + ROW_VEC + 4 * k + i:256 + ROW_VEC + 4 * k + i + 1, :] = jnp.sum(sums[i], axis=0, keepdims=True)

    def add4(a, b):
        return tuple(x + y for x, y in zip(a, b))

    par4[256:512, :] = jnp.zeros((256, LAT), F32)

    def grid_embed(i, c):
        rows = blk(i, BLK_G)
        out, hid, dsilu, nrm, inv = mlp_fwd(0, mm_tn(grid_in[:, rows], w_grid_in[...]))
        grid_lat[rows, :] = out.astype(BF16)
        hid0[rows, :] = hid
        ds0[rows, :] = dsilu
        nm0[rows, :] = nrm
        iv0[rows, :] = inv
        return c

    loop('grid_embed', 0, n_grid // BLK_G, grid_embed, 0)

    def row_pair(i):
        return jnp.concatenate([send_rows[2 * i:2 * i + 1, :], send_rows[2 * i + 1:2 * i + 2, :]], axis=1)

    def columns_of(row):
        return jnp.transpose(jnp.broadcast_to(row, (128, 128)))

    def one_hot(col, n):
        lane = lax.broadcasted_iota(jnp.int32, (128, 128), 1).astype(jnp.int16)
        col = col.astype(jnp.int16)
        return jnp.concatenate([jnp.where(col == lane + jnp.full((), 128 * t, jnp.int16), jnp.ones((), BF16), jnp.zeros((), BF16)) for t in range(n // 128)], axis=1)

    def one_hot_t(row, n):
        sub = lax.broadcasted_iota(jnp.int32, (n, 128), 0).astype(jnp.int16)
        return jnp.where(sub == jnp.broadcast_to(row, (n, 128)).astype(jnp.int16), jnp.ones((), BF16), jnp.zeros((), BF16))

    for i in range(N_DEV // 2):
        pick = one_hot(columns_of(row_pair(i)), n_grid)
        outgoing[128 * i:128 * (i + 1), :] = mm(pick, grid_lat[...]).astype(BF16)

    with jax.named_scope('w_bar'):
        pl.semaphore_wait(barrier, N_DEV - 1)
    fwd = exchange(outgoing, incoming, f_send, f_recv)

    def grid_update(i, sums):
        rows = blk(i, BLK_G)
        lat = grid_lat[rows, :]
        out, hid, dsilu, nrm, inv = mlp_fwd(5, mm(lat, w_grid_up[...]))
        grid_out[rows, :] = (lat.astype(F32) + out).astype(BF16)
        d_out = d_grid_out[rows, :].astype(F32)
        d_lin, d_pre, add = mlp_bwd(5, dsilu, nrm, inv, d_out)
        hid5[rows, :] = hid
        dl_g[rows, :] = d_lin
        dp_g[rows, :] = d_pre
        d_grid_lat[rows, :] = d_out + mm_nt(d_pre, w_grid_up[...])
        return add4(sums, add)

    put_vec(5, loop('grid_update', 0, n_grid // BLK_G, grid_update, zeros4))
    par0[0:256, :] = mm_tn(grid_lat[...], dp_g[...])
    par0[256:512, :] = mm_tn(hid5[...], dl_g[...])
    stage0(0)

    def mesh_embed(i, c):
        rows = blk(i, BLK_M)
        out, hid, dsilu, nrm, inv = mlp_fwd(1, mm_tn(mesh_static[:, rows], w_mesh_in[...]))
        mesh_lat[rows, :] = out.astype(BF16)
        hid1[rows, :] = hid
        ds1[rows, :] = dsilu
        nm1[rows, :] = nrm
        iv1[rows, :] = inv
        return c

    loop('mesh_embed', 0, n_mesh // BLK_M, mesh_embed, 0)

    def hots(i, c):
        rows = blk(i, 128)
        src = edge_src[pl.ds(i, 1), :]
        dst = edge_dst[pl.ds(i, 1), :]
        oh_src[rows, :] = one_hot(columns_of(src), n_grid)
        oh_dst[rows, :] = one_hot(columns_of(dst), n_mesh)
        oht_src[:, rows] = one_hot_t(src, n_grid)
        oht_dst[:, rows] = one_hot_t(dst, n_mesh)
        return c

    loop('hots', 0, n_edge // 128, hots, 0)
    stage1(0)

    def edge_embed(i, c):
        rows = blk(i, BLK_E)
        out, hid, dsilu, nrm, inv = mlp_fwd(2, mm_tn(edge_static[:, rows], w_edge_in[...]))
        lat = out.astype(BF16)
        edge_lat[rows, :] = lat
        hid2[rows, :] = hid
        ds2[rows, :] = dsilu
        nm2[rows, :] = nrm
        iv2[rows, :] = inv
        recv = mm(oh_dst[rows, :], mesh_lat[...]).astype(BF16)
        part3[rows, :] = mm(lat, w_edge_up[0:LAT, :]) + mm(recv, w_edge_up[2 * LAT:3 * LAT, :])
        return c

    loop('edge_embed', 0, n_edge // BLK_E, edge_embed, 0)
    stage2(0)

    with jax.named_scope('w_fwd'):
        for copy in fwd:
            copy.wait_recv()

    def edge_update(i, c):
        rows = blk(i, BLK_E)
        sender = mm(oh_src[rows, :], incoming[...]).astype(BF16)
        out, hid, dsilu, nrm, inv = mlp_fwd(3, part3[rows, :] + mm(sender, w_edge_up[LAT:2 * LAT, :]))
        edge_new[rows, :] = (edge_lat[rows, :].astype(F32) + out).astype(BF16)
        hid3[rows, :] = hid
        ds3[rows, :] = dsilu
        nm3[rows, :] = nrm
        iv3[rows, :] = inv
        return c

    loop('edge_update', 0, n_edge // BLK_E, edge_update, 0)
    stage3(0)

    def mesh_update(i, sums):
        rows = blk(i, BLK_M)
        total = mm(oht_dst[rows, :], edge_new[...]).astype(BF16)
        agg[rows, :] = total
        lat = mesh_lat[rows, :]
        out, hid, dsilu, nrm, inv = mlp_fwd(4, mm(lat, w_mesh_up[0:LAT, :]) + mm(total, w_mesh_up[LAT:2 * LAT, :]))
        mesh_out[rows, :] = (lat.astype(F32) + out).astype(BF16)
        d_out = d_mesh_out[rows, :].astype(F32)
        d_lin, d_pre, add = mlp_bwd(4, dsilu, nrm, inv, d_out)
        hid4[rows, :] = hid
        dl_m[rows, :] = d_lin
        dp_m[rows, :] = d_pre
        d_mesh_lat[rows, :] = d_out + mm_nt(d_pre, w_mesh_up[0:LAT, :])
        d_agg[rows, :] = mm_nt(d_pre, w_mesh_up[LAT:2 * LAT, :]).astype(BF16)
        return add4(sums, add)

    put_vec(4, loop('mesh_update', 0, n_mesh // BLK_M, mesh_update, zeros4))
    par1[0:256, :] = mm_tn(mesh_lat[...], dp_m[...])
    par1[256:512, :] = mm_tn(agg[...], dp_m[...])
    par1[512:768, :] = mm_tn(hid4[...], dl_m[...])
    stage0(1)

    def edge_back(i, sums):
        rows = blk(i, BLK_E)
        d_out = mm(oh_dst[rows, :], d_agg[...])
        d_lin, d_pre, add = mlp_bwd(3, ds3[rows, :], nm3[rows, :], iv3[rows, :], d_out)
        dl_e[rows, :] = d_lin
        dp_e[rows, :] = d_pre
        part3[rows, :] = d_out + mm_nt(d_pre, w_edge_up[0:LAT, :])
        return add4(sums, add)

    half_way = (n_edge // BLK_E + 1) // 2
    sums3 = loop('edge_back', 0, half_way, edge_back, zeros4)
    stage1(1)
    put_vec(3, loop('edge_back', half_way, n_edge // BLK_E, edge_back, sums3))

    def slot_back(i, c):
        rows = blk(i, BLK_S)
        d_sum = mm(oht_src[rows, :], dp_e[...]).astype(BF16)
        d_slot[rows, :] = d_sum
        d_incoming[rows, :] = mm_nt(d_sum, w_edge_up[LAT:2 * LAT, :]).astype(BF16)
        return c

    loop('slot_back', 0, n_grid // BLK_S, slot_back, 0)
    bwd = exchange(d_incoming, d_outgoing, b_send, b_recv)

    def node_back(i, c):
        rows = blk(i, BLK_M)
        d_sum = mm(oht_dst[rows, :], dp_e[...]).astype(BF16)
        d_node[rows, :] = d_sum
        d_mesh_lat[rows, :] = d_mesh_lat[rows, :] + mm_nt(d_sum, w_edge_up[2 * LAT:3 * LAT, :])
        return c

    loop('node_back', 0, n_mesh // BLK_M, node_back, 0)
    par2[0:256, :] = mm_tn(edge_lat[...], dp_e[...])
    par2[256:512, :] = mm_tn(incoming[...], d_slot[...])
    par2[512:768, :] = mm_tn(mesh_lat[...], d_node[...])
    par2[768:1024, :] = mm_tn(hid3[...], dl_e[...])
    stage0(2)

    def mesh_in_back(i, sums):
        rows = blk(i, BLK_M)
        d_lin, d_pre, add = mlp_bwd(1, ds1[rows, :], nm1[rows, :], iv1[rows, :], d_mesh_lat[rows, :])
        dl_m[rows, :] = d_lin
        dp_m[rows, :] = d_pre
        return add4(sums, add)

    put_vec(1, loop('mesh_in_back', 0, n_mesh // BLK_M, mesh_in_back, zeros4))
    stage1(2)

    def edge_in_back(i, sums):
        rows = blk(i, BLK_E)
        d_lin, d_pre, add = mlp_bwd(2, ds2[rows, :], nm2[rows, :], iv2[rows, :], part3[rows, :])
        dl_e[rows, :] = d_lin
        dp_e[rows, :] = d_pre
        return add4(sums, add)

    put_vec(2, loop('edge_in_back', 0, n_edge // BLK_E, edge_in_back, zeros4))
    par3[0:256, :] = mm_tn(hid2[...], dl_e[...])
    par3[256:512, :] = mm_tn(hid1[...], dl_m[...])
    stage0(3)
    stage2(1)
    par4[256 + ROW_EDGE_IN:256 + ROW_EDGE_IN + 4, :] = mm(edge_static[...], dp_e[...])
    par4[256 + ROW_MESH_IN:256 + ROW_MESH_IN + 3, :] = mm(mesh_static[...], dp_m[...])
    stage1(3)

    with jax.named_scope('w_bwd'):
        for copy in bwd:
            copy.wait_recv()

    all_rows = jnp.concatenate([row_pair(i) for i in range(N_DEV // 2)], axis=1)

    def grid_in_back(i, sums):
        rows = blk(i, BLK_G)
        sub = lax.broadcasted_iota(jnp.int32, (BLK_G, N_DEV * slots), 0) + i * BLK_G
        spread = jnp.where(sub == all_rows, 1.0, 0.0).astype(BF16)
        d_out = d_grid_lat[rows, :] + mm(spread, d_outgoing[...])
        d_lin, d_pre, add = mlp_bwd(0, ds0[rows, :], nm0[rows, :], iv0[rows, :], d_out)
        dl_g[rows, :] = d_lin
        dp_g[rows, :] = d_pre
        d_grid_in[:, rows] = mm_nt(w_grid_in[...], d_pre)
        return add4(sums, add)

    put_vec(0, loop('grid_in_back', 0, n_grid // BLK_G, grid_in_back, zeros4))
    with jax.named_scope("dw0"):
        par4[0:256, :] = mm_tn(hid0[...], dl_g[...])
        par4[256:256 + grid_in.shape[0], :] = mm(grid_in[...], dp_g[...])
        stage0(4)
    stage2(2)
    stage1(4)
    stage2(3)
    stage3(1)
    stage2(4)
    stage3(2)
    stage3(3)
    stage3(4)
    for g in range(N_GROUP):
        stage4(g)
    with jax.named_scope("t_send"):
        for copy in pending:
            copy.wait_send()


def final_kernel(mesh_res, grid_res, d_grid_res, res0, res1, res2, res3, res4,
                 mesh_out, grid_out, d_grid_in, d_w_grid_in, d_w_mesh_in, d_w_edge_in, d_w_edge_up, d_w_mesh_up, d_w_grid_up, d_w_second, d_vectors):
    mesh_out[...] = mesh_res[...]
    grid_out[...] = grid_res[...]
    d_grid_in[...] = d_grid_res[...]
    d_w_grid_up[...] = res0[0:256, :].astype(F32)
    d_w_second[5] = res0[256:512, :].astype(F32)
    d_w_mesh_up[...] = res1[0:512, :].astype(F32)
    d_w_second[4] = res1[512:768, :].astype(F32)
    d_w_edge_up[...] = res2[0:768, :].astype(F32)
    d_w_second[3] = res2[768:1024, :].astype(F32)
    d_w_second[2] = res3[0:256, :].astype(F32)
    d_w_second[1] = res3[256:512, :].astype(F32)
    d_w_second[0] = res4[0:256, :].astype(F32)
    small = res4[256:512, :].astype(F32)
    d_w_grid_in[...] = small[0:d_w_grid_in.shape[0], :]
    d_w_edge_in[...] = small[ROW_EDGE_IN:ROW_EDGE_IN + 4, :]
    d_w_mesh_in[...] = small[ROW_MESH_IN:ROW_MESH_IN + 3, :]
    d_vectors[...] = small[ROW_VEC:ROW_VEC + 24, :].reshape(6, 4, LAT)


def solution(mesh):
    row_spec = P(AXIS_NAME, None)
    edge_spec = P(AXIS_NAME)
    rep_spec = P()
    in_specs = (row_spec, row_spec, row_spec, row_spec, edge_spec, edge_spec) + (rep_spec,) * 8 + (row_spec, row_spec)
    out_specs = (row_spec, row_spec, row_spec) + (rep_spec,) * 8

    def local_step(grid_in, mesh_static, edge_static, send_rows, edge_src, edge_dst, *rest):
        n_grid, feats = grid_in.shape
        n_mesh = mesh_static.shape[0]
        n_edge = edge_static.shape[0]
        n_slot = send_rows.size
        src2 = edge_src.reshape(n_edge // 128, 128)
        dst2 = edge_dst.reshape(n_edge // 128, 128)

        def vm(shape, dtype):
            return pltpu.VMEM(shape, dtype)

        def rows_bf(n):
            return vm((n, LAT), BF16)

        def rows_f32(n):
            return vm((n, LAT), F32)

        dma = pltpu.SemaphoreType.DMA
        scratch = [
            rows_bf(n_grid), rows_bf(n_mesh), rows_bf(n_edge), rows_bf(n_slot), rows_bf(n_slot), rows_bf(n_slot), rows_bf(n_slot),
            vm((n_edge, n_slot), BF16), vm((n_slot, n_edge), BF16), vm((n_edge, n_mesh), BF16), vm((n_mesh, n_edge), BF16),
            rows_bf(n_grid), rows_bf(n_mesh), rows_bf(n_edge), rows_bf(n_edge), rows_bf(n_mesh), rows_bf(n_grid),
            rows_f32(n_grid), rows_f32(n_mesh), rows_f32(n_edge), rows_f32(n_edge),
            rows_f32(n_grid), rows_f32(n_mesh), rows_f32(n_edge), rows_f32(n_edge),
            vm((n_grid, 1), F32), vm((n_mesh, 1), F32), vm((n_edge, 1), F32), vm((n_edge, 1), F32),
            rows_f32(n_edge), rows_bf(n_edge), rows_bf(n_mesh), rows_f32(n_grid), rows_f32(n_mesh), rows_bf(n_mesh), rows_bf(n_slot), rows_bf(n_mesh),
            rows_bf(n_grid), rows_bf(n_grid), rows_bf(n_mesh), rows_bf(n_mesh), rows_bf(n_edge), rows_bf(n_edge),
        ]
        scratch += [rows_f32(r) for r in GROUP_ROWS]
        scratch += [rows_f32(r // 2) for r in GROUP_ROWS]
        scratch += [rows_bf(r // 2) for r in GROUP_ROWS]
        scratch += [vm((7, r // 16, LAT), BF16) for r in GROUP_ROWS]
        scratch += [dma((16,)), dma((16,)), dma((16,)), dma((16,)), ] + [dma((N_GROUP,)), dma((N_GROUP,)), dma((N_GROUP, 8)), dma((N_GROUP, 8)), dma((N_GROUP, 8)), dma((N_GROUP, 8)), dma((N_GROUP,)), dma((N_GROUP,))]
        shape = jax.ShapeDtypeStruct
        outs = (shape((n_mesh, LAT), BF16), shape((n_grid, LAT), BF16), shape((feats, n_grid), F32)) + tuple(shape((r, LAT), BF16) for r in GROUP_ROWS)
        vspec = pl.BlockSpec(memory_space=pltpu.VMEM)
        results = pl.pallas_call(
            main_kernel,
            out_shape=outs,
            in_specs=[vspec] * 16,
            out_specs=tuple([vspec] * len(outs)),
            scratch_shapes=scratch,
            compiler_params=pltpu.CompilerParams(collective_id=0, has_side_effects=True, vmem_limit_bytes=47 * 1024 * 1024),
        )(grid_in.T, mesh_static.T, edge_static.T, send_rows, src2, dst2, *rest)

        finals = (shape((n_mesh, LAT), BF16), shape((n_grid, LAT), BF16), shape((feats, n_grid), F32),
                  shape((feats, LAT), F32), shape((3, LAT), F32), shape((4, LAT), F32), shape((3 * LAT, LAT), F32),
                  shape((2 * LAT, LAT), F32), shape((LAT, LAT), F32), shape((6, LAT, LAT), F32), shape((6, 4, LAT), F32))
        done = pl.pallas_call(
            final_kernel,
            out_shape=finals,
            in_specs=[vspec] * len(outs),
            out_specs=tuple([vspec] * len(finals)),
            compiler_params=pltpu.CompilerParams(vmem_limit_bytes=16 * 1024 * 1024),
        )(*results)
        return done[:2] + (done[2].T,) + done[3:]

    return jax.shard_map(local_step, mesh=mesh, in_specs=in_specs, out_specs=out_specs, check_vma=False)
```

```python
import functools

import jax
import jax.numpy as jnp
from jax import lax
from jax.experimental import pallas as pl
from jax.experimental.pallas import tpu as pltpu
from jax.sharding import PartitionSpec as P

LN_EPS = 1e-5
AXIS_NAME = 'gp'
N_DEV = 16
N_CHIP = 8
LAT = 256
BLK_G, BLK_M, BLK_E, BLK_S = 1024, 512, 768, 512
F32 = jnp.float32
BF16 = jnp.bfloat16

GROUP_ROWS = (512, 768, 1024, 512, 512)
N_GROUP = len(GROUP_ROWS)
ROW_EDGE_IN = 168
ROW_MESH_IN = 176
ROW_VEC = 184


def mm(a, b):
    return lax.dot_general(a, b, (((1,), (0,)), ((), ())), preferred_element_type=F32)


def mm_nt(a, b):
    return lax.dot_general(a, b, (((1,), (1,)), ((), ())), preferred_element_type=F32)


def mm_tn(a, b):
    return lax.dot_general(a, b, (((0,), (0,)), ((), ())), preferred_element_type=F32)


def fold8(x):
    return jnp.sum(x.reshape(-1, 8, x.shape[-1]), axis=0)


def main_kernel(
        hbm_grid_in, hbm_mesh_static, hbm_edge_static, hbm_send_rows, hbm_edge_src, hbm_edge_dst,
        hbm_w_grid_in, hbm_w_mesh_in, hbm_w_edge_in, hbm_w_edge_up, hbm_w_mesh_up, hbm_w_grid_up, hbm_w_second, hbm_vectors, hbm_d_mesh_out, hbm_d_grid_out,
        mesh_out, grid_out, d_grid_in, res0, res1, res2, res3, res4,
        grid_in, mesh_static, edge_static, send_rows, edge_src, edge_dst, w_grid_in, w_mesh_in, w_edge_in, w_edge_up, w_mesh_up, w_grid_up, w_second, vectors, d_mesh_out, d_grid_out, in_sem,
        grid_lat, mesh_lat, edge_lat, outgoing, incoming, d_incoming, d_outgoing,
        oh_src, oht_src, oh_dst, oht_dst,
        hid0, hid1, hid2, hid3, hid4, hid5,
        ds0, ds1, ds2, ds3, nm0, nm1, nm2, nm3, iv0, iv1, iv2, iv3,
        part3, edge_new, agg, d_grid_lat, d_mesh_lat, d_agg, d_slot, d_node,
        dl_g, dp_g, dl_m, dp_m, dl_e, dp_e,
        par0, par1, par2, par3, par4, ra0, ra1, ra2, ra3, ra4, cs0, cs1, cs2, cs3, cs4, rb0, rb1, rb2, rb3, rb4,
        f_send, f_recv, b_send, b_recv, s0_send, s0_recv, s1_send, s1_recv, s2_send, s2_recv, s3_send, s3_recv):
    me = lax.axis_index(AXIS_NAME)
    core = me % 2
    chip = me // 2
    n_grid = grid_lat.shape[0]
    n_mesh = mesh_lat.shape[0]
    n_edge = edge_lat.shape[0]
    slots = send_rows.shape[1]
    pars, ras, css = (par0, par1, par2, par3, par4), (ra0, ra1, ra2, ra3, ra4), (cs0, cs1, cs2, cs3, cs4)
    rbs, ress = (rb0, rb1, rb2, rb3, rb4), (res0, res1, res2, res3, res4)

    def flip(idx, j):
        out = 0
        for b in range(4):
            bit = (idx // (1 << b)) % 2
            out = out + (1 << b) * (1 - bit if (j >> b) & 1 else bit)
        return out

    def loop(name, lo, hi, body, init):
        with jax.named_scope(name):
            return lax.fori_loop(lo, hi, body, init)

    barrier = pltpu.get_barrier_semaphore()
    for j in range(1, N_DEV):
        pl.semaphore_signal(barrier, inc=1, device_id=(flip(me, j),), device_id_type=pl.DeviceIdType.MESH)

    order = ('send_rows', 'grid_in', 'w_grid_in', 'vectors', 'w_second', 'w_grid_up', 'd_grid_out', 'mesh_static', 'w_mesh_in', 'edge_src',
             'edge_dst', 'edge_static', 'w_edge_in', 'w_edge_up', 'w_mesh_up', 'd_mesh_out')
    loads = {
        'grid_in': (hbm_grid_in, grid_in),
        'mesh_static': (hbm_mesh_static, mesh_static),
        'edge_static': (hbm_edge_static, edge_static),
        'send_rows': (hbm_send_rows, send_rows),
        'edge_src': (hbm_edge_src, edge_src),
        'edge_dst': (hbm_edge_dst, edge_dst),
        'w_grid_in': (hbm_w_grid_in, w_grid_in),
        'w_mesh_in': (hbm_w_mesh_in, w_mesh_in),
        'w_edge_in': (hbm_w_edge_in, w_edge_in),
        'w_edge_up': (hbm_w_edge_up, w_edge_up),
        'w_mesh_up': (hbm_w_mesh_up, w_mesh_up),
        'w_grid_up': (hbm_w_grid_up, w_grid_up),
        'w_second': (hbm_w_second, w_second),
        'vectors': (hbm_vectors, vectors),
        'd_mesh_out': (hbm_d_mesh_out, d_mesh_out),
        'd_grid_out': (hbm_d_grid_out, d_grid_out),
    }
    for i, name in enumerate(order):
        loads[name] = pltpu.make_async_copy(loads[name][0], loads[name][1], in_sem.at[i])
        loads[name].start()

    def need(*which):
        for name in which:
            loads[name].wait()

    pending = []

    def send(src, dst, send_sem, recv_sem, dev):
        copy = pltpu.make_async_remote_copy(src_ref=src, dst_ref=dst, send_sem=send_sem, recv_sem=recv_sem,
                                            device_id=(dev,), device_id_type=pl.DeviceIdType.MESH)
        copy.start()
        pending.append(copy)
        return copy

    far, near = (15, 14, 11, 10, 13, 12, 9, 8), (7, 6, 3, 2, 5, 4, 1)
    z_bit = me // 8
    chip_order = (7, 3, 5, 6, 1, 2, 4)

    def exchange(src, dst, send_sem, recv_sem, peers):
        copies = []
        for j in peers:
            peer = flip(me, j)
            copies.append(send(src.at[pl.ds(pl.multiple_of(peer * slots, slots), slots)],
                               dst.at[pl.ds(pl.multiple_of(me * slots, slots), slots)],
                               send_sem.at[j], recv_sem.at[j], peer))
        if peers is near:
            mine = pl.ds(pl.multiple_of(me * slots, slots), slots)
            dst[mine, :] = src[mine, :]
        return copies

    live = {}

    def stage0(g):
        half = GROUP_ROWS[g] // 2
        other = pl.ds(pl.multiple_of((1 - core) * half, half), half)
        live[g] = [send(pars[g].at[other], ras[g], s0_send.at[g], s0_recv.at[g], flip(me, 1))]

    def stage1(g):
        with jax.named_scope('s1_%d' % g):
            live[g][0].wait_recv()
            half = GROUP_ROWS[g] // 2
            part = half // N_CHIP
            mine = pl.ds(pl.multiple_of(core * half, half), half)
            total = pars[g][mine, :] + ras[g][...]
            ras[g][...] = total
            css[g][...] = total.astype(BF16)
            copies = []
            for j in chip_order:
                peer = flip(me, 2 * j)
                copies.append(send(css[g].at[pl.ds(pl.multiple_of((peer // 2) * part, part), part)], rbs[g].at[j - 1],
                                   s1_send.at[g, j], s1_recv.at[g, j], peer))
            live[g] = copies

    def stage2(g):
        with jax.named_scope('s2_%d' % g):
            half = GROUP_ROWS[g] // 2
            part = half // N_CHIP
            for copy in live[g]:
                copy.wait_recv()
            total = ras[g][pl.ds(pl.multiple_of(chip * part, part), part), :]
            for j in range(1, N_CHIP):
                total = total + rbs[g][j - 1].astype(F32)
            mine = pl.ds(pl.multiple_of(core * half + chip * part, part), part)
            ress[g][mine, :] = total.astype(BF16)
            copies = []
            for j in chip_order:
                copies.append(send(ress[g].at[mine], ress[g].at[mine], s2_send.at[g, j], s2_recv.at[g, j], flip(me, 2 * j)))
            live[g] = copies

    def stage3(g):
        with jax.named_scope('s3_%d' % g):
            half = GROUP_ROWS[g] // 2
            for copy in live[g]:
                copy.wait_recv()
            mine = pl.ds(pl.multiple_of(core * half, half), half)
            live[g] = [send(ress[g].at[mine], ress[g].at[mine], s3_send.at[g], s3_recv.at[g], flip(me, 1))]

    def stage4(g):
        with jax.named_scope('s4_%d' % g):
            live[g][0].wait_recv()

    def blk(i, size):
        return pl.ds(pl.multiple_of(i * size, size), size)

    def vec(k, i):
        return vectors[k, i:i + 1, :]

    def mlp_fwd(k, pre):
        x = pre + vec(k, 0)
        sig = jax.nn.sigmoid(x)
        act = x * sig
        hid = act.astype(BF16)
        o = mm(hid, w_second[k]) + vec(k, 1)
        cen = o - jnp.mean(o, axis=-1, keepdims=True)
        inv = lax.rsqrt(jnp.mean(cen * cen, axis=-1, keepdims=True) + LN_EPS)
        nrm = cen * inv
        out = nrm * vec(k, 2) + vec(k, 3)
        dsilu = sig + act * (1.0 - sig)
        return out, hid, dsilu, nrm, inv

    def mlp_bwd(k, dsilu, nrm, inv, d_out):
        dn = d_out * vec(k, 2)
        m1 = jnp.mean(dn, axis=-1, keepdims=True)
        m2 = jnp.mean(dn * nrm, axis=-1, keepdims=True)
        d_lin = inv * (dn - m1 - nrm * m2)
        d_lin_bf = d_lin.astype(BF16)
        d_pre = mm_nt(d_lin_bf, w_second[k]) * dsilu
        return d_lin_bf, d_pre.astype(BF16), (fold8(d_pre), fold8(d_lin), fold8(d_out * nrm), fold8(d_out))

    zeros4 = tuple(jnp.zeros((8, LAT), F32) for _ in range(4))

    def put_vec(k, sums):
        for i in range(4):
            par4[256 + ROW_VEC + 4 * k + i:256 + ROW_VEC + 4 * k + i + 1, :] = jnp.sum(sums[i], axis=0, keepdims=True)

    def add4(a, b):
        return tuple(x + y for x, y in zip(a, b))

    par4[256:512, :] = jnp.zeros((256, LAT), F32)

    need('grid_in', 'w_grid_in', 'vectors', 'w_second')

    def grid_embed(i, c):
        rows = blk(i, BLK_G)
        out, hid, dsilu, nrm, inv = mlp_fwd(0, mm_tn(grid_in[:, rows], w_grid_in[...]))
        grid_lat[rows, :] = out.astype(BF16)
        hid0[rows, :] = hid
        ds0[rows, :] = dsilu
        nm0[rows, :] = nrm
        iv0[rows, :] = inv
        return c

    loop('grid_embed', 0, n_grid // BLK_G, grid_embed, 0)

    def row_pair(i):
        return jnp.concatenate([send_rows[pl.ds(2 * i, 1), :], send_rows[pl.ds(2 * i + 1, 1), :]], axis=1)

    def columns_of(row):
        return jnp.transpose(jnp.broadcast_to(row, (128, 128)))

    def one_hot(col, n):
        lane = lax.broadcasted_iota(jnp.int32, (128, 128), 1).astype(jnp.int16)
        col = col.astype(jnp.int16)
        return jnp.concatenate([jnp.where(col == lane + jnp.full((), 128 * t, jnp.int16), jnp.ones((), BF16), jnp.zeros((), BF16)) for t in range(n // 128)], axis=1)

    def one_hot_t(row, n):
        sub = lax.broadcasted_iota(jnp.int32, (n, 128), 0).astype(jnp.int16)
        return jnp.where(sub == jnp.broadcast_to(row, (n, 128)).astype(jnp.int16), jnp.ones((), BF16), jnp.zeros((), BF16))

    need('send_rows')
    def gather_half(half):
        for t in range(N_DEV // 4):
            i = half * (N_DEV // 4) + t
            pick = one_hot(columns_of(row_pair(i)), n_grid)
            outgoing[blk(i, 128), :] = mm(pick, grid_lat[...]).astype(BF16)

    gather_half(1 - z_bit)
    with jax.named_scope('w_bar'):
        pl.semaphore_wait(barrier, N_DEV - 1)
    fwd = exchange(outgoing, incoming, f_send, f_recv, far)
    gather_half(z_bit)
    fwd += exchange(outgoing, incoming, f_send, f_recv, near)

    need('w_grid_up', 'd_grid_out')

    def grid_update(i, sums):
        rows = blk(i, BLK_G)
        lat = grid_lat[rows, :]
        out, hid, dsilu, nrm, inv = mlp_fwd(5, mm(lat, w_grid_up[...]))
        grid_out[rows, :] = (lat.astype(F32) + out).astype(BF16)
        d_out = d_grid_out[rows, :].astype(F32)
        d_lin, d_pre, add = mlp_bwd(5, dsilu, nrm, inv, d_out)
        hid5[rows, :] = hid
        dl_g[rows, :] = d_lin
        dp_g[rows, :] = d_pre
        d_grid_lat[rows, :] = d_out + mm_nt(d_pre, w_grid_up[...])
        return add4(sums, add)

    put_vec(5, loop('grid_update', 0, n_grid // BLK_G, grid_update, zeros4))
    par0[0:256, :] = mm_tn(grid_lat[...], dp_g[...])
    par0[256:512, :] = mm_tn(hid5[...], dl_g[...])
    stage0(0)

    need('mesh_static', 'w_mesh_in', 'edge_src', 'edge_dst', 'edge_static', 'w_edge_in', 'w_edge_up')

    def mesh_embed(i, c):
        rows = blk(i, BLK_M)
        out, hid, dsilu, nrm, inv = mlp_fwd(1, mm_tn(mesh_static[:, rows], w_mesh_in[...]))
        mesh_lat[rows, :] = out.astype(BF16)
        hid1[rows, :] = hid
        ds1[rows, :] = dsilu
        nm1[rows, :] = nrm
        iv1[rows, :] = inv
        return c

    loop('mesh_embed', 0, n_mesh // BLK_M, mesh_embed, 0)

    def hots(i, c):
        rows = blk(i, 128)
        src = edge_src[pl.ds(i, 1), :]
        dst = edge_dst[pl.ds(i, 1), :]
        oh_src[rows, :] = one_hot(columns_of(src), n_grid)
        oh_dst[rows, :] = one_hot(columns_of(dst), n_mesh)
        oht_src[:, rows] = one_hot_t(src, n_grid)
        oht_dst[:, rows] = one_hot_t(dst, n_mesh)
        return c

    loop('hots', 0, n_edge // 128, hots, 0)
    stage1(0)

    def edge_embed(i, c):
        rows = blk(i, BLK_E)
        out, hid, dsilu, nrm, inv = mlp_fwd(2, mm_tn(edge_static[:, rows], w_edge_in[...]))
        lat = out.astype(BF16)
        edge_lat[rows, :] = lat
        hid2[rows, :] = hid
        ds2[rows, :] = dsilu
        nm2[rows, :] = nrm
        iv2[rows, :] = inv
        recv = mm(oh_dst[rows, :], mesh_lat[...]).astype(BF16)
        part3[rows, :] = mm(lat, w_edge_up[0:LAT, :]) + mm(recv, w_edge_up[2 * LAT:3 * LAT, :])
        return c

    loop('edge_embed', 0, n_edge // BLK_E, edge_embed, 0)

    with jax.named_scope('w_fwd'):
        for copy in fwd:
            copy.wait_recv()

    def edge_update(i, c):
        rows = blk(i, BLK_E)
        sender = mm(oh_src[rows, :], incoming[...]).astype(BF16)
        out, hid, dsilu, nrm, inv = mlp_fwd(3, part3[rows, :] + mm(sender, w_edge_up[LAT:2 * LAT, :]))
        edge_new[rows, :] = (edge_lat[rows, :].astype(F32) + out).astype(BF16)
        hid3[rows, :] = hid
        ds3[rows, :] = dsilu
        nm3[rows, :] = nrm
        iv3[rows, :] = inv
        return c

    loop('edge_update', 0, n_edge // BLK_E, edge_update, 0)
    stage2(0)

    need('w_mesh_up', 'd_mesh_out')

    def mesh_update(i, sums):
        rows = blk(i, BLK_M)
        total = mm(oht_dst[rows, :], edge_new[...]).astype(BF16)
        agg[rows, :] = total
        lat = mesh_lat[rows, :]
        out, hid, dsilu, nrm, inv = mlp_fwd(4, mm(lat, w_mesh_up[0:LAT, :]) + mm(total, w_mesh_up[LAT:2 * LAT, :]))
        mesh_out[rows, :] = (lat.astype(F32) + out).astype(BF16)
        d_out = d_mesh_out[rows, :].astype(F32)
        d_lin, d_pre, add = mlp_bwd(4, dsilu, nrm, inv, d_out)
        hid4[rows, :] = hid
        dl_m[rows, :] = d_lin
        dp_m[rows, :] = d_pre
        d_mesh_lat[rows, :] = d_out + mm_nt(d_pre, w_mesh_up[0:LAT, :])
        d_agg[rows, :] = mm_nt(d_pre, w_mesh_up[LAT:2 * LAT, :]).astype(BF16)
        return add4(sums, add)

    put_vec(4, loop('mesh_update', 0, n_mesh // BLK_M, mesh_update, zeros4))
    par1[0:256, :] = mm_tn(mesh_lat[...], dp_m[...])
    par1[256:512, :] = mm_tn(agg[...], dp_m[...])
    par1[512:768, :] = mm_tn(hid4[...], dl_m[...])
    stage0(1)

    def edge_back(i, sums):
        rows = blk(i, BLK_E)
        d_out = mm(oh_dst[rows, :], d_agg[...])
        d_lin, d_pre, add = mlp_bwd(3, ds3[rows, :], nm3[rows, :], iv3[rows, :], d_out)
        dl_e[rows, :] = d_lin
        dp_e[rows, :] = d_pre
        part3[rows, :] = d_out + mm_nt(d_pre, w_edge_up[0:LAT, :])
        return add4(sums, add)

    put_vec(3, loop('edge_back', 0, n_edge // BLK_E, edge_back, zeros4))
    stage1(1)

    def slot_back(i, c):
        rows = blk(i, BLK_S)
        d_sum = mm(oht_src[rows, :], dp_e[...]).astype(BF16)
        d_slot[rows, :] = d_sum
        d_incoming[rows, :] = mm_nt(d_sum, w_edge_up[LAT:2 * LAT, :]).astype(BF16)
        return c

    with jax.named_scope('slot_back'):
        slot_back(1 - z_bit, 0)
    bwd = exchange(d_incoming, d_outgoing, b_send, b_recv, far)
    with jax.named_scope('slot_back'):
        slot_back(z_bit, 0)
    bwd += exchange(d_incoming, d_outgoing, b_send, b_recv, near)

    def node_back(i, c):
        rows = blk(i, BLK_M)
        d_sum = mm(oht_dst[rows, :], dp_e[...]).astype(BF16)
        d_node[rows, :] = d_sum
        d_mesh_lat[rows, :] = d_mesh_lat[rows, :] + mm_nt(d_sum, w_edge_up[2 * LAT:3 * LAT, :])
        return c

    loop('node_back', 0, n_mesh // BLK_M, node_back, 0)
    par2[0:256, :] = mm_tn(edge_lat[...], dp_e[...])
    par2[256:512, :] = mm_tn(incoming[...], d_slot[...])
    par2[512:768, :] = mm_tn(mesh_lat[...], d_node[...])
    par2[768:1024, :] = mm_tn(hid3[...], dl_e[...])
    stage0(2)

    def mesh_in_back(i, sums):
        rows = blk(i, BLK_M)
        d_lin, d_pre, add = mlp_bwd(1, ds1[rows, :], nm1[rows, :], iv1[rows, :], d_mesh_lat[rows, :])
        dl_m[rows, :] = d_lin
        dp_m[rows, :] = d_pre
        return add4(sums, add)

    put_vec(1, loop('mesh_in_back', 0, n_mesh // BLK_M, mesh_in_back, zeros4))
    def edge_in_back(i, sums):
        rows = blk(i, BLK_E)
        d_lin, d_pre, add = mlp_bwd(2, ds2[rows, :], nm2[rows, :], iv2[rows, :], part3[rows, :])
        dl_e[rows, :] = d_lin
        dp_e[rows, :] = d_pre
        return add4(sums, add)

    put_vec(2, loop('edge_in_back', 0, n_edge // BLK_E, edge_in_back, zeros4))
    par3[0:256, :] = mm_tn(hid2[...], dl_e[...])
    par3[256:512, :] = mm_tn(hid1[...], dl_m[...])
    stage0(3)
    stage1(2)
    stage2(1)
    stage3(0)
    par4[256 + ROW_EDGE_IN:256 + ROW_EDGE_IN + 4, :] = mm(edge_static[...], dp_e[...])
    par4[256 + ROW_MESH_IN:256 + ROW_MESH_IN + 3, :] = mm(mesh_static[...], dp_m[...])
    stage1(3)

    with jax.named_scope('w_bwd'):
        for copy in bwd:
            copy.wait_recv()

    all_rows = jnp.concatenate([row_pair(i) for i in range(N_DEV // 2)], axis=1)

    def grid_in_back(i, sums):
        rows = blk(i, BLK_G)
        sub = lax.broadcasted_iota(jnp.int32, (BLK_G, N_DEV * slots), 0) + i * BLK_G
        spread = jnp.where(sub == all_rows, 1.0, 0.0).astype(BF16)
        d_out = d_grid_lat[rows, :] + mm(spread, d_outgoing[...])
        d_lin, d_pre, add = mlp_bwd(0, ds0[rows, :], nm0[rows, :], iv0[rows, :], d_out)
        dl_g[rows, :] = d_lin
        dp_g[rows, :] = d_pre
        d_grid_in[:, rows] = mm_nt(w_grid_in[...], d_pre)
        return add4(sums, add)

    put_vec(0, loop('grid_in_back', 0, n_grid // BLK_G, grid_in_back, zeros4))
    with jax.named_scope("dw0"):
        par4[0:256, :] = mm_tn(hid0[...], dl_g[...])
        par4[256:256 + grid_in.shape[0], :] = mm(grid_in[...], dp_g[...])
        stage0(4)
    stage1(4)
    stage2(2)
    stage2(3)
    stage3(1)
    stage2(4)
    stage3(2)
    stage3(3)
    stage3(4)
    for g in range(N_GROUP):
        stage4(g)
    with jax.named_scope("t_send"):
        for copy in pending:
            copy.wait_send()


def final_kernel(mesh_res, grid_res, d_grid_res, res0, res1, res2, res3, res4,
                 mesh_out, grid_out, d_grid_in, d_w_grid_in, d_w_mesh_in, d_w_edge_in, d_w_edge_up, d_w_mesh_up, d_w_grid_up, d_w_second, d_vectors):
    mesh_out[...] = mesh_res[...]
    grid_out[...] = grid_res[...]
    d_grid_in[...] = d_grid_res[...]
    d_w_grid_up[...] = res0[0:256, :].astype(F32)
    d_w_second[5] = res0[256:512, :].astype(F32)
    d_w_mesh_up[...] = res1[0:512, :].astype(F32)
    d_w_second[4] = res1[512:768, :].astype(F32)
    d_w_edge_up[...] = res2[0:768, :].astype(F32)
    d_w_second[3] = res2[768:1024, :].astype(F32)
    d_w_second[2] = res3[0:256, :].astype(F32)
    d_w_second[1] = res3[256:512, :].astype(F32)
    d_w_second[0] = res4[0:256, :].astype(F32)
    small = res4[256:512, :].astype(F32)
    d_w_grid_in[...] = small[0:d_w_grid_in.shape[0], :]
    d_w_edge_in[...] = small[ROW_EDGE_IN:ROW_EDGE_IN + 4, :]
    d_w_mesh_in[...] = small[ROW_MESH_IN:ROW_MESH_IN + 3, :]
    d_vectors[...] = small[ROW_VEC:ROW_VEC + 24, :].reshape(6, 4, LAT)


def solution(mesh):
    row_spec = P(AXIS_NAME, None)
    edge_spec = P(AXIS_NAME)
    rep_spec = P()
    in_specs = (row_spec, row_spec, row_spec, row_spec, edge_spec, edge_spec) + (rep_spec,) * 8 + (row_spec, row_spec)
    out_specs = (row_spec, row_spec, row_spec) + (rep_spec,) * 8

    def local_step(grid_in, mesh_static, edge_static, send_rows, edge_src, edge_dst, *rest):
        n_grid, feats = grid_in.shape
        n_mesh = mesh_static.shape[0]
        n_edge = edge_static.shape[0]
        n_slot = send_rows.size
        src2 = edge_src.reshape(n_edge // 128, 128)
        dst2 = edge_dst.reshape(n_edge // 128, 128)

        def vm(shape, dtype):
            return pltpu.VMEM(shape, dtype)

        def rows_bf(n):
            return vm((n, LAT), BF16)

        def rows_f32(n):
            return vm((n, LAT), F32)

        dma = pltpu.SemaphoreType.DMA
        args = (grid_in.T, mesh_static.T, edge_static.T, send_rows, src2, dst2) + rest
        scratch = [vm(a.shape, a.dtype) for a in args] + [dma((len(args),))]
        scratch += [
            rows_bf(n_grid), rows_bf(n_mesh), rows_bf(n_edge), rows_bf(n_slot), rows_bf(n_slot), rows_bf(n_slot), rows_bf(n_slot),
            vm((n_edge, n_slot), BF16), vm((n_slot, n_edge), BF16), vm((n_edge, n_mesh), BF16), vm((n_mesh, n_edge), BF16),
            rows_bf(n_grid), rows_bf(n_mesh), rows_bf(n_edge), rows_bf(n_edge), rows_bf(n_mesh), rows_bf(n_grid),
            rows_f32(n_grid), rows_f32(n_mesh), rows_f32(n_edge), rows_f32(n_edge),
            rows_f32(n_grid), rows_f32(n_mesh), rows_f32(n_edge), rows_f32(n_edge),
            vm((n_grid, 1), F32), vm((n_mesh, 1), F32), vm((n_edge, 1), F32), vm((n_edge, 1), F32),
            rows_f32(n_edge), rows_bf(n_edge), rows_bf(n_mesh), rows_f32(n_grid), rows_f32(n_mesh), rows_bf(n_mesh), rows_bf(n_slot), rows_bf(n_mesh),
            rows_bf(n_grid), rows_bf(n_grid), rows_bf(n_mesh), rows_bf(n_mesh), rows_bf(n_edge), rows_bf(n_edge),
        ]
        scratch += [rows_f32(r) for r in GROUP_ROWS]
        scratch += [rows_f32(r // 2) for r in GROUP_ROWS]
        scratch += [rows_bf(r // 2) for r in GROUP_ROWS]
        scratch += [vm((7, r // 16, LAT), BF16) for r in GROUP_ROWS]
        scratch += [dma((16,)), dma((16,)), dma((16,)), dma((16,)), ] + [dma((N_GROUP,)), dma((N_GROUP,)), dma((N_GROUP, 8)), dma((N_GROUP, 8)), dma((N_GROUP, 8)), dma((N_GROUP, 8)), dma((N_GROUP,)), dma((N_GROUP,))]
        shape = jax.ShapeDtypeStruct
        outs = (shape((n_mesh, LAT), BF16), shape((n_grid, LAT), BF16), shape((feats, n_grid), F32)) + tuple(shape((r, LAT), BF16) for r in GROUP_ROWS)
        vspec = pl.BlockSpec(memory_space=pltpu.VMEM)
        results = pl.pallas_call(
            main_kernel,
            out_shape=tuple(pltpu.VMEM(o.shape, o.dtype) for o in outs),
            in_specs=[pl.BlockSpec(memory_space=pltpu.MemorySpace.HBM)] * 16,
            out_specs=tuple([vspec] * len(outs)),
            scratch_shapes=scratch,
            compiler_params=pltpu.CompilerParams(collective_id=0, has_side_effects=True, vmem_limit_bytes=62300 * 1024),
        )(*args)

        finals = (shape((n_mesh, LAT), BF16), shape((n_grid, LAT), BF16), shape((feats, n_grid), F32),
                  shape((feats, LAT), F32), shape((3, LAT), F32), shape((4, LAT), F32), shape((3 * LAT, LAT), F32),
                  shape((2 * LAT, LAT), F32), shape((LAT, LAT), F32), shape((6, LAT, LAT), F32), shape((6, 4, LAT), F32))
        done = pl.pallas_call(
            final_kernel,
            out_shape=finals,
            in_specs=[vspec] * len(outs),
            out_specs=tuple([vspec] * len(finals)),
            compiler_params=pltpu.CompilerParams(vmem_limit_bytes=16 * 1024 * 1024),
        )(*results)
        return done[:2] + (done[2].T,) + done[3:]

    return jax.shard_map(local_step, mesh=mesh, in_specs=in_specs, out_specs=out_specs, check_vma=False)
```

```python
import functools

import jax
import jax.numpy as jnp
from jax import lax
from jax.experimental import pallas as pl
from jax.experimental.pallas import tpu as pltpu
from jax.sharding import PartitionSpec as P

LN_EPS = 1e-5
AXIS_NAME = 'gp'
N_DEV = 16
N_CHIP = 8
LAT = 256
BLK_G, BLK_M, BLK_E, BLK_S = 1024, 512, 768, 512
F32 = jnp.float32
BF16 = jnp.bfloat16

GROUP_ROWS = (512, 768, 1024, 512, 512)
N_GROUP = len(GROUP_ROWS)
ROW_EDGE_IN = 168
ROW_MESH_IN = 176
ROW_VEC = 184


def mm(a, b):
    return lax.dot_general(a, b, (((1,), (0,)), ((), ())), preferred_element_type=F32)


def mm_nt(a, b):
    return lax.dot_general(a, b, (((1,), (1,)), ((), ())), preferred_element_type=F32)


def mm_tn(a, b):
    return lax.dot_general(a, b, (((0,), (0,)), ((), ())), preferred_element_type=F32)


def fold8(x):
    return jnp.sum(x.reshape(-1, 8, x.shape[-1]), axis=0)


def main_kernel(
        hbm_grid_in, hbm_mesh_static, hbm_edge_static, hbm_send_rows, hbm_edge_src, hbm_edge_dst,
        hbm_w_grid_in, hbm_w_mesh_in, hbm_w_edge_in, hbm_w_edge_up, hbm_w_mesh_up, hbm_w_grid_up, hbm_w_second, hbm_vectors, hbm_d_mesh_out, hbm_d_grid_out,
        mesh_out, grid_out, d_grid_in, res0, res1, res2, res3, res4,
        grid_in, mesh_static, edge_static, send_rows, edge_src, edge_dst, w_grid_in, w_mesh_in, w_edge_in, w_edge_up, w_mesh_up, w_grid_up, w_second, vectors, d_mesh_out, d_grid_out, in_sem,
        grid_lat, mesh_lat, edge_lat, outgoing, incoming, d_incoming, d_outgoing,
        oh_src, oht_src, oh_dst, oht_dst,
        hid0, hid1, hid2, hid3, hid4, hid5,
        ds0, ds1, ds2, ds3, nm0, nm1, nm2, nm3, iv0, iv1, iv2, iv3,
        part3, edge_new, agg, d_grid_lat, d_mesh_lat, d_agg, d_slot, d_node,
        dl_g, dp_g, dl_m, dp_m, dl_e, dp_e,
        par0, par1, par2, par3, par4, ra0, ra1, ra2, ra3, ra4, cs0, cs1, cs2, cs3, cs4, rb0, rb1, rb2, rb3, rb4,
        f_send, f_recv, b_send, b_recv, s0_send, s0_recv, s1_send, s1_recv, s2_send, s2_recv, s3_send, s3_recv):
    me = lax.axis_index(AXIS_NAME)
    core = me % 2
    chip = me // 2
    n_grid = grid_lat.shape[0]
    n_mesh = mesh_lat.shape[0]
    n_edge = edge_lat.shape[0]
    slots = send_rows.shape[1]
    pars, ras, css = (par0, par1, par2, par3, par4), (ra0, ra1, ra2, ra3, ra4), (cs0, cs1, cs2, cs3, cs4)
    rbs, ress = (rb0, rb1, rb2, rb3, rb4), (res0, res1, res2, res3, res4)

    def flip(idx, j):
        out = 0
        for b in range(4):
            bit = (idx // (1 << b)) % 2
            out = out + (1 << b) * (1 - bit if (j >> b) & 1 else bit)
        return out

    def loop(name, lo, hi, body, init):
        with jax.named_scope(name):
            return lax.fori_loop(lo, hi, body, init)

    barrier = pltpu.get_barrier_semaphore()
    for j in range(1, N_DEV):
        pl.semaphore_signal(barrier, inc=1, device_id=(flip(me, j),), device_id_type=pl.DeviceIdType.MESH)

    order = ('send_rows', 'grid_in', 'w_grid_in', 'vectors', 'w_second', 'w_grid_up', 'd_grid_out', 'mesh_static', 'w_mesh_in', 'edge_src',
             'edge_dst', 'edge_static', 'w_edge_in', 'w_edge_up', 'w_mesh_up', 'd_mesh_out')
    loads = {
        'grid_in': (hbm_grid_in, grid_in),
        'mesh_static': (hbm_mesh_static, mesh_static),
        'edge_static': (hbm_edge_static, edge_static),
        'send_rows': (hbm_send_rows, send_rows),
        'edge_src': (hbm_edge_src, edge_src),
        'edge_dst': (hbm_edge_dst, edge_dst),
        'w_grid_in': (hbm_w_grid_in, w_grid_in),
        'w_mesh_in': (hbm_w_mesh_in, w_mesh_in),
        'w_edge_in': (hbm_w_edge_in, w_edge_in),
        'w_edge_up': (hbm_w_edge_up, w_edge_up),
        'w_mesh_up': (hbm_w_mesh_up, w_mesh_up),
        'w_grid_up': (hbm_w_grid_up, w_grid_up),
        'w_second': (hbm_w_second, w_second),
        'vectors': (hbm_vectors, vectors),
        'd_mesh_out': (hbm_d_mesh_out, d_mesh_out),
        'd_grid_out': (hbm_d_grid_out, d_grid_out),
    }
    for i, name in enumerate(order):
        loads[name] = pltpu.make_async_copy(loads[name][0], loads[name][1], in_sem.at[i])
        loads[name].start()

    def need(*which):
        for name in which:
            loads[name].wait()

    pending = []

    def send(src, dst, send_sem, recv_sem, dev):
        copy = pltpu.make_async_remote_copy(src_ref=src, dst_ref=dst, send_sem=send_sem, recv_sem=recv_sem,
                                            device_id=(dev,), device_id_type=pl.DeviceIdType.MESH)
        copy.start()

    def settle(ref, sem):
        pltpu.make_async_copy(ref, ref, sem).wait()

    far, near = (15, 14, 11, 10, 13, 12, 9, 8), (7, 6, 3, 2, 5, 4, 1)
    z_bit = me // 8
    chip_order = (7, 3, 5, 6, 1, 2, 4)

    def exchange(src, dst, send_sem, recv_sem, peers):
        for j in peers:
            peer = flip(me, j)
            send(src.at[pl.ds(pl.multiple_of(peer * slots, slots), slots)],
                 dst.at[pl.ds(pl.multiple_of(me * slots, slots), slots)], send_sem, recv_sem, peer)
        if peers is near:
            mine = pl.ds(pl.multiple_of(me * slots, slots), slots)
            dst[mine, :] = src[mine, :]
            pending.append((src.at[pl.ds(0, (N_DEV - 1) * slots)], send_sem))

    def stage0(g):
        half = GROUP_ROWS[g] // 2
        other = pl.ds(pl.multiple_of((1 - core) * half, half), half)
        send(pars[g].at[other], ras[g], s0_send.at[g], s0_recv.at[g], flip(me, 1))
        pending.append((ras[g], s0_send.at[g]))

    def stage1(g):
        with jax.named_scope('s1_%d' % g):
            settle(ras[g], s0_recv.at[g])
            half = GROUP_ROWS[g] // 2
            part = half // N_CHIP
            mine = pl.ds(pl.multiple_of(core * half, half), half)
            total = pars[g][mine, :] + ras[g][...]
            ras[g][...] = total
            css[g][...] = total.astype(BF16)
            for j in chip_order:
                peer = flip(me, 2 * j)
                send(css[g].at[pl.ds(pl.multiple_of((peer // 2) * part, part), part)], rbs[g].at[j - 1],
                     s1_send.at[g], s1_recv.at[g], peer)
            pending.append((rbs[g], s1_send.at[g]))

    def stage2(g):
        with jax.named_scope('s2_%d' % g):
            half = GROUP_ROWS[g] // 2
            part = half // N_CHIP
            settle(rbs[g], s1_recv.at[g])
            total = ras[g][pl.ds(pl.multiple_of(chip * part, part), part), :]
            for j in range(1, N_CHIP):
                total = total + rbs[g][j - 1].astype(F32)
            mine = pl.ds(pl.multiple_of(core * half + chip * part, part), part)
            ress[g][mine, :] = total.astype(BF16)
            for j in chip_order:
                send(ress[g].at[mine], ress[g].at[mine], s2_send.at[g], s2_recv.at[g], flip(me, 2 * j))
            pending.append((rbs[g], s2_send.at[g]))

    def stage3(g):
        with jax.named_scope('s3_%d' % g):
            half = GROUP_ROWS[g] // 2
            settle(rbs[g], s2_recv.at[g])
            mine = pl.ds(pl.multiple_of(core * half, half), half)
            send(ress[g].at[mine], ress[g].at[mine], s3_send.at[g], s3_recv.at[g], flip(me, 1))
            pending.append((css[g], s3_send.at[g]))

    def stage4(g):
        with jax.named_scope('s4_%d' % g):
            settle(css[g], s3_recv.at[g])

    def blk(i, size):
        return pl.ds(pl.multiple_of(i * size, size), size)

    def vec(k, i):
        return vectors[k, i:i + 1, :]

    def mlp_fwd(k, pre):
        x = pre + vec(k, 0)
        sig = jax.nn.sigmoid(x)
        act = x * sig
        hid = act.astype(BF16)
        o = mm(hid, w_second[k]) + vec(k, 1)
        cen = o - jnp.mean(o, axis=-1, keepdims=True)
        inv = lax.rsqrt(jnp.mean(cen * cen, axis=-1, keepdims=True) + LN_EPS)
        nrm = cen * inv
        out = nrm * vec(k, 2) + vec(k, 3)
        dsilu = sig + act * (1.0 - sig)
        return out, hid, dsilu, nrm, inv

    def mlp_bwd(k, dsilu, nrm, inv, d_out):
        dn = d_out * vec(k, 2)
        m1 = jnp.mean(dn, axis=-1, keepdims=True)
        m2 = jnp.mean(dn * nrm, axis=-1, keepdims=True)
        d_lin = inv * (dn - m1 - nrm * m2)
        d_lin_bf = d_lin.astype(BF16)
        d_pre = mm_nt(d_lin_bf, w_second[k]) * dsilu
        return d_lin_bf, d_pre.astype(BF16), (fold8(d_pre), fold8(d_lin), fold8(d_out * nrm), fold8(d_out))

    zeros4 = tuple(jnp.zeros((8, LAT), F32) for _ in range(4))

    def put_vec(k, sums):
        for i in range(4):
            par4[256 + ROW_VEC + 4 * k + i:256 + ROW_VEC + 4 * k + i + 1, :] = jnp.sum(sums[i], axis=0, keepdims=True)

    def add4(a, b):
        return tuple(x + y for x, y in zip(a, b))

    par4[256:512, :] = jnp.zeros((256, LAT), F32)

    need('grid_in', 'w_grid_in', 'vectors', 'w_second')

    def grid_embed(i, c):
        rows = blk(i, BLK_G)
        out, hid, dsilu, nrm, inv = mlp_fwd(0, mm_tn(grid_in[:, rows], w_grid_in[...]))
        grid_lat[rows, :] = out.astype(BF16)
        hid0[rows, :] = hid
        ds0[rows, :] = dsilu
        nm0[rows, :] = nrm
        iv0[rows, :] = inv
        return c

    loop('grid_embed', 0, n_grid // BLK_G, grid_embed, 0)

    def row_pair(i):
        return jnp.concatenate([send_rows[pl.ds(2 * i, 1), :], send_rows[pl.ds(2 * i + 1, 1), :]], axis=1)

    def columns_of(row):
        return jnp.transpose(jnp.broadcast_to(row, (128, 128)))

    def one_hot(col, n):
        lane = lax.broadcasted_iota(jnp.int32, (128, 128), 1).astype(jnp.int16)
        col = col.astype(jnp.int16)
        return jnp.concatenate([jnp.where(col == lane + jnp.full((), 128 * t, jnp.int16), jnp.ones((), BF16), jnp.zeros((), BF16)) for t in range(n // 128)], axis=1)

    def one_hot_t(row, n):
        sub = lax.broadcasted_iota(jnp.int32, (n, 128), 0).astype(jnp.int16)
        return jnp.where(sub == jnp.broadcast_to(row, (n, 128)).astype(jnp.int16), jnp.ones((), BF16), jnp.zeros((), BF16))

    need('send_rows')
    def gather_half(half):
        for t in range(N_DEV // 4):
            i = half * (N_DEV // 4) + t
            pick = one_hot(columns_of(row_pair(i)), n_grid)
            outgoing[blk(i, 128), :] = mm(pick, grid_lat[...]).astype(BF16)

    gather_half(1 - z_bit)
    with jax.named_scope('w_bar'):
        pl.semaphore_wait(barrier, N_DEV - 1)
    exchange(outgoing, incoming, f_send, f_recv, far)
    gather_half(z_bit)
    exchange(outgoing, incoming, f_send, f_recv, near)

    need('w_grid_up', 'd_grid_out')

    def grid_update(i, sums):
        rows = blk(i, BLK_G)
        lat = grid_lat[rows, :]
        out, hid, dsilu, nrm, inv = mlp_fwd(5, mm(lat, w_grid_up[...]))
        grid_out[rows, :] = (lat.astype(F32) + out).astype(BF16)
        d_out = d_grid_out[rows, :].astype(F32)
        d_lin, d_pre, add = mlp_bwd(5, dsilu, nrm, inv, d_out)
        hid5[rows, :] = hid
        dl_g[rows, :] = d_lin
        dp_g[rows, :] = d_pre
        d_grid_lat[rows, :] = d_out + mm_nt(d_pre, w_grid_up[...])
        return add4(sums, add)

    put_vec(5, loop('grid_update', 0, n_grid // BLK_G, grid_update, zeros4))
    par0[0:256, :] = mm_tn(grid_lat[...], dp_g[...])
    par0[256:512, :] = mm_tn(hid5[...], dl_g[...])
    stage0(0)

    need('mesh_static', 'w_mesh_in', 'edge_src', 'edge_dst', 'edge_static', 'w_edge_in', 'w_edge_up')

    def mesh_embed(i, c):
        rows = blk(i, BLK_M)
        out, hid, dsilu, nrm, inv = mlp_fwd(1, mm_tn(mesh_static[:, rows], w_mesh_in[...]))
        mesh_lat[rows, :] = out.astype(BF16)
        hid1[rows, :] = hid
        ds1[rows, :] = dsilu
        nm1[rows, :] = nrm
        iv1[rows, :] = inv
        return c

    loop('mesh_embed', 0, n_mesh // BLK_M, mesh_embed, 0)

    def hots(i, c):
        rows = blk(i, 128)
        src = edge_src[pl.ds(i, 1), :]
        dst = edge_dst[pl.ds(i, 1), :]
        oh_src[rows, :] = one_hot(columns_of(src), n_grid)
        oh_dst[rows, :] = one_hot(columns_of(dst), n_mesh)
        oht_src[:, rows] = one_hot_t(src, n_grid)
        oht_dst[:, rows] = one_hot_t(dst, n_mesh)
        return c

    loop('hots', 0, n_edge // 128, hots, 0)
    stage1(0)

    def edge_embed(i, c):
        rows = blk(i, BLK_E)
        out, hid, dsilu, nrm, inv = mlp_fwd(2, mm_tn(edge_static[:, rows], w_edge_in[...]))
        lat = out.astype(BF16)
        edge_lat[rows, :] = lat
        hid2[rows, :] = hid
        ds2[rows, :] = dsilu
        nm2[rows, :] = nrm
        iv2[rows, :] = inv
        recv = mm(oh_dst[rows, :], mesh_lat[...]).astype(BF16)
        part3[rows, :] = mm(lat, w_edge_up[0:LAT, :]) + mm(recv, w_edge_up[2 * LAT:3 * LAT, :])
        return c

    loop('edge_embed', 0, n_edge // BLK_E, edge_embed, 0)

    with jax.named_scope('w_fwd'):
        settle(incoming.at[pl.ds(0, (N_DEV - 1) * slots)], f_recv)

    def edge_update(i, c):
        rows = blk(i, BLK_E)
        sender = mm(oh_src[rows, :], incoming[...]).astype(BF16)
        out, hid, dsilu, nrm, inv = mlp_fwd(3, part3[rows, :] + mm(sender, w_edge_up[LAT:2 * LAT, :]))
        edge_new[rows, :] = (edge_lat[rows, :].astype(F32) + out).astype(BF16)
        hid3[rows, :] = hid
        ds3[rows, :] = dsilu
        nm3[rows, :] = nrm
        iv3[rows, :] = inv
        return c

    loop('edge_update', 0, n_edge // BLK_E, edge_update, 0)
    stage2(0)

    need('w_mesh_up', 'd_mesh_out')

    def mesh_update(i, sums):
        rows = blk(i, BLK_M)
        total = mm(oht_dst[rows, :], edge_new[...]).astype(BF16)
        agg[rows, :] = total
        lat = mesh_lat[rows, :]
        out, hid, dsilu, nrm, inv = mlp_fwd(4, mm(lat, w_mesh_up[0:LAT, :]) + mm(total, w_mesh_up[LAT:2 * LAT, :]))
        mesh_out[rows, :] = (lat.astype(F32) + out).astype(BF16)
        d_out = d_mesh_out[rows, :].astype(F32)
        d_lin, d_pre, add = mlp_bwd(4, dsilu, nrm, inv, d_out)
        hid4[rows, :] = hid
        dl_m[rows, :] = d_lin
        dp_m[rows, :] = d_pre
        d_mesh_lat[rows, :] = d_out + mm_nt(d_pre, w_mesh_up[0:LAT, :])
        d_agg[rows, :] = mm_nt(d_pre, w_mesh_up[LAT:2 * LAT, :]).astype(BF16)
        return add4(sums, add)

    put_vec(4, loop('mesh_update', 0, n_mesh // BLK_M, mesh_update, zeros4))
    par1[0:256, :] = mm_tn(mesh_lat[...], dp_m[...])
    par1[256:512, :] = mm_tn(agg[...], dp_m[...])
    par1[512:768, :] = mm_tn(hid4[...], dl_m[...])
    stage0(1)

    def edge_back(i, sums):
        rows = blk(i, BLK_E)
        d_out = mm(oh_dst[rows, :], d_agg[...])
        d_lin, d_pre, add = mlp_bwd(3, ds3[rows, :], nm3[rows, :], iv3[rows, :], d_out)
        dl_e[rows, :] = d_lin
        dp_e[rows, :] = d_pre
        part3[rows, :] = d_out + mm_nt(d_pre, w_edge_up[0:LAT, :])
        return add4(sums, add)

    put_vec(3, loop('edge_back', 0, n_edge // BLK_E, edge_back, zeros4))
    stage1(1)

    def slot_back(i, c):
        rows = blk(i, BLK_S)
        d_sum = mm(oht_src[rows, :], dp_e[...]).astype(BF16)
        d_slot[rows, :] = d_sum
        d_incoming[rows, :] = mm_nt(d_sum, w_edge_up[LAT:2 * LAT, :]).astype(BF16)
        return c

    with jax.named_scope('slot_back'):
        slot_back(1 - z_bit, 0)
    exchange(d_incoming, d_outgoing, b_send, b_recv, far)
    with jax.named_scope('slot_back'):
        slot_back(z_bit, 0)
    exchange(d_incoming, d_outgoing, b_send, b_recv, near)

    def node_back(i, c):
        rows = blk(i, BLK_M)
        d_sum = mm(oht_dst[rows, :], dp_e[...]).astype(BF16)
        d_node[rows, :] = d_sum
        d_mesh_lat[rows, :] = d_mesh_lat[rows, :] + mm_nt(d_sum, w_edge_up[2 * LAT:3 * LAT, :])
        return c

    loop('node_back', 0, n_mesh // BLK_M, node_back, 0)
    par2[0:256, :] = mm_tn(edge_lat[...], dp_e[...])
    par2[256:512, :] = mm_tn(incoming[...], d_slot[...])
    par2[512:768, :] = mm_tn(mesh_lat[...], d_node[...])
    par2[768:1024, :] = mm_tn(hid3[...], dl_e[...])
    stage0(2)

    def mesh_in_back(i, sums):
        rows = blk(i, BLK_M)
        d_lin, d_pre, add = mlp_bwd(1, ds1[rows, :], nm1[rows, :], iv1[rows, :], d_mesh_lat[rows, :])
        dl_m[rows, :] = d_lin
        dp_m[rows, :] = d_pre
        return add4(sums, add)

    put_vec(1, loop('mesh_in_back', 0, n_mesh // BLK_M, mesh_in_back, zeros4))
    def edge_in_back(i, sums):
        rows = blk(i, BLK_E)
        d_lin, d_pre, add = mlp_bwd(2, ds2[rows, :], nm2[rows, :], iv2[rows, :], part3[rows, :])
        dl_e[rows, :] = d_lin
        dp_e[rows, :] = d_pre
        return add4(sums, add)

    put_vec(2, loop('edge_in_back', 0, n_edge // BLK_E, edge_in_back, zeros4))
    par3[0:256, :] = mm_tn(hid2[...], dl_e[...])
    par3[256:512, :] = mm_tn(hid1[...], dl_m[...])
    stage0(3)
    stage1(2)
    stage2(1)
    stage3(0)
    par4[256 + ROW_EDGE_IN:256 + ROW_EDGE_IN + 4, :] = mm(edge_static[...], dp_e[...])
    par4[256 + ROW_MESH_IN:256 + ROW_MESH_IN + 3, :] = mm(mesh_static[...], dp_m[...])
    stage1(3)

    with jax.named_scope('w_bwd'):
        settle(d_outgoing.at[pl.ds(0, (N_DEV - 1) * slots)], b_recv)

    all_rows = jnp.concatenate([row_pair(i) for i in range(N_DEV // 2)], axis=1)

    def grid_in_back(i, sums):
        rows = blk(i, BLK_G)
        sub = lax.broadcasted_iota(jnp.int32, (BLK_G, N_DEV * slots), 0) + i * BLK_G
        spread = jnp.where(sub == all_rows, 1.0, 0.0).astype(BF16)
        d_out = d_grid_lat[rows, :] + mm(spread, d_outgoing[...])
        d_lin, d_pre, add = mlp_bwd(0, ds0[rows, :], nm0[rows, :], iv0[rows, :], d_out)
        dl_g[rows, :] = d_lin
        dp_g[rows, :] = d_pre
        d_grid_in[:, rows] = mm_nt(w_grid_in[...], d_pre)
        return add4(sums, add)

    put_vec(0, loop('grid_in_back', 0, n_grid // BLK_G, grid_in_back, zeros4))
    with jax.named_scope("dw0"):
        par4[0:256, :] = mm_tn(hid0[...], dl_g[...])
        par4[256:256 + grid_in.shape[0], :] = mm(grid_in[...], dp_g[...])
        stage0(4)
    stage1(4)
    stage2(2)
    stage2(3)
    stage3(1)
    stage2(4)
    stage3(2)
    stage3(3)
    stage3(4)
    for g in range(N_GROUP):
        stage4(g)
    with jax.named_scope("t_send"):
        for ref, sem in pending:
            settle(ref, sem)


def final_kernel(mesh_res, grid_res, d_grid_res, res0, res1, res2, res3, res4,
                 mesh_out, grid_out, d_grid_in, d_w_grid_in, d_w_mesh_in, d_w_edge_in, d_w_edge_up, d_w_mesh_up, d_w_grid_up, d_w_second, d_vectors,
                 b_grid_in, b_mesh_in, b_edge_in, b_edge_up, b_mesh_up, b_grid_up, b_second, b_vectors, sems):
    plan = []
    started = []

    def start(src, dst):
        copy = pltpu.make_async_copy(src, dst, sems.at[len(started)])
        copy.start()
        started.append(copy)

    def put(src, rows, buf, dst):
        buf[...] = src[rows[0]:rows[1], :].astype(F32)
        plan.append((buf, dst))
        if len(plan) > 1:
            start(*plan[-2])

    start(d_grid_res, d_grid_in)
    start(grid_res, grid_out)
    start(mesh_res, mesh_out)
    put(res2, (0, 768), b_edge_up, d_w_edge_up)
    put(res1, (0, 512), b_mesh_up, d_w_mesh_up)
    put(res0, (0, 256), b_grid_up, d_w_grid_up)
    put(res0, (256, 512), b_second.at[5], d_w_second.at[5])
    put(res1, (512, 768), b_second.at[4], d_w_second.at[4])
    put(res2, (768, 1024), b_second.at[3], d_w_second.at[3])
    put(res3, (0, 256), b_second.at[2], d_w_second.at[2])
    put(res3, (256, 512), b_second.at[1], d_w_second.at[1])
    put(res4, (0, 256), b_second.at[0], d_w_second.at[0])
    small = res4[256:512, :].astype(F32)
    b_edge_in[...] = small[ROW_EDGE_IN:ROW_EDGE_IN + 4, :]
    b_mesh_in[...] = small[ROW_MESH_IN:ROW_MESH_IN + 3, :]
    b_vectors[...] = small[ROW_VEC:ROW_VEC + 24, :].reshape(6, 4, LAT)
    b_grid_in[...] = small[0:b_grid_in.shape[0], :]
    start(*plan[-1])
    start(b_edge_in, d_w_edge_in)
    start(b_mesh_in, d_w_mesh_in)
    start(b_vectors, d_vectors)
    start(b_grid_in, d_w_grid_in)
    for copy in started:
        copy.wait()


def solution(mesh):
    row_spec = P(AXIS_NAME, None)
    edge_spec = P(AXIS_NAME)
    rep_spec = P()
    in_specs = (row_spec, row_spec, row_spec, row_spec, edge_spec, edge_spec) + (rep_spec,) * 8 + (row_spec, row_spec)
    out_specs = (row_spec, row_spec, row_spec) + (rep_spec,) * 8

    def local_step(grid_in, mesh_static, edge_static, send_rows, edge_src, edge_dst, *rest):
        n_grid, feats = grid_in.shape
        n_mesh = mesh_static.shape[0]
        n_edge = edge_static.shape[0]
        n_slot = send_rows.size
        src2 = edge_src.reshape(n_edge // 128, 128)
        dst2 = edge_dst.reshape(n_edge // 128, 128)

        def vm(shape, dtype):
            return pltpu.VMEM(shape, dtype)

        def rows_bf(n):
            return vm((n, LAT), BF16)

        def rows_f32(n):
            return vm((n, LAT), F32)

        dma = pltpu.SemaphoreType.DMA
        args = (grid_in.T, mesh_static.T, edge_static.T, send_rows, src2, dst2) + rest
        scratch = [vm(a.shape, a.dtype) for a in args] + [dma((len(args),))]
        scratch += [
            rows_bf(n_grid), rows_bf(n_mesh), rows_bf(n_edge), rows_bf(n_slot), rows_bf(n_slot), rows_bf(n_slot), rows_bf(n_slot),
            vm((n_edge, n_slot), BF16), vm((n_slot, n_edge), BF16), vm((n_edge, n_mesh), BF16), vm((n_mesh, n_edge), BF16),
            rows_bf(n_grid), rows_bf(n_mesh), rows_bf(n_edge), rows_bf(n_edge), rows_bf(n_mesh), rows_bf(n_grid),
            rows_f32(n_grid), rows_f32(n_mesh), rows_f32(n_edge), rows_f32(n_edge),
            rows_f32(n_grid), rows_f32(n_mesh), rows_f32(n_edge), rows_f32(n_edge),
            vm((n_grid, 1), F32), vm((n_mesh, 1), F32), vm((n_edge, 1), F32), vm((n_edge, 1), F32),
            rows_f32(n_edge), rows_bf(n_edge), rows_bf(n_mesh), rows_f32(n_grid), rows_f32(n_mesh), rows_bf(n_mesh), rows_bf(n_slot), rows_bf(n_mesh),
            rows_bf(n_grid), rows_bf(n_grid), rows_bf(n_mesh), rows_bf(n_mesh), rows_bf(n_edge), rows_bf(n_edge),
        ]
        scratch += [rows_f32(r) for r in GROUP_ROWS]
        scratch += [rows_f32(r // 2) for r in GROUP_ROWS]
        scratch += [rows_bf(r // 2) for r in GROUP_ROWS]
        scratch += [vm((7, r // 16, LAT), BF16) for r in GROUP_ROWS]
        scratch += [dma] * 4 + [dma((N_GROUP,))] * 8
        shape = jax.ShapeDtypeStruct
        outs = (shape((n_mesh, LAT), BF16), shape((n_grid, LAT), BF16), shape((feats, n_grid), F32)) + tuple(shape((r, LAT), BF16) for r in GROUP_ROWS)
        vspec = pl.BlockSpec(memory_space=pltpu.VMEM)
        results = pl.pallas_call(
            main_kernel,
            out_shape=tuple(pltpu.VMEM(o.shape, o.dtype) for o in outs),
            in_specs=[pl.BlockSpec(memory_space=pltpu.MemorySpace.HBM)] * 16,
            out_specs=tuple([vspec] * len(outs)),
            scratch_shapes=scratch,
            compiler_params=pltpu.CompilerParams(collective_id=0, has_side_effects=True, vmem_limit_bytes=62300 * 1024),
        )(*args)

        finals = (shape((n_mesh, LAT), BF16), shape((n_grid, LAT), BF16), shape((feats, n_grid), F32),
                  shape((feats, LAT), F32), shape((3, LAT), F32), shape((4, LAT), F32), shape((3 * LAT, LAT), F32),
                  shape((2 * LAT, LAT), F32), shape((LAT, LAT), F32), shape((6, LAT, LAT), F32), shape((6, 4, LAT), F32))
        done = pl.pallas_call(
            final_kernel,
            out_shape=finals,
            in_specs=[vspec] * len(outs),
            out_specs=tuple([pl.BlockSpec(memory_space=pltpu.MemorySpace.HBM)] * len(finals)),
            scratch_shapes=[vm(f.shape, f.dtype) for f in finals[3:]] + [dma((16,))],
            compiler_params=pltpu.CompilerParams(vmem_limit_bytes=16 * 1024 * 1024),
        )(*results)
        return done[:2] + (done[2].T,) + done[3:]

    return jax.shard_map(local_step, mesh=mesh, in_specs=in_specs, out_specs=out_specs, check_vma=False)
```

```python
import functools

import jax
import jax.numpy as jnp
from jax import lax
from jax.experimental import pallas as pl
from jax.experimental.pallas import tpu as pltpu
from jax.sharding import PartitionSpec as P

LN_EPS = 1e-5
AXIS_NAME = 'gp'
N_DEV = 16
N_CHIP = 8
LAT = 256
BLK_G, BLK_M, BLK_E, BLK_S = 1024, 512, 768, 512
F32 = jnp.float32
BF16 = jnp.bfloat16

GROUP_ROWS = (512, 768, 1024, 512, 512)
N_GROUP = len(GROUP_ROWS)
RELAYED = (1, 2, 3)
ROW_EDGE_IN = 168
ROW_MESH_IN = 176
ROW_VEC = 184


def mm(a, b):
    return lax.dot_general(a, b, (((1,), (0,)), ((), ())), preferred_element_type=F32)


def mm_nt(a, b):
    return lax.dot_general(a, b, (((1,), (1,)), ((), ())), preferred_element_type=F32)


def mm_tn(a, b):
    return lax.dot_general(a, b, (((0,), (0,)), ((), ())), preferred_element_type=F32)


def fold8(x):
    return jnp.sum(x.reshape(-1, 8, x.shape[-1]), axis=0)


def main_kernel(
        hbm_grid_in, hbm_mesh_static, hbm_edge_static, hbm_send_rows, hbm_edge_src, hbm_edge_dst,
        hbm_w_grid_in, hbm_w_mesh_in, hbm_w_edge_in, hbm_w_edge_up, hbm_w_mesh_up, hbm_w_grid_up, hbm_w_second, hbm_vectors, hbm_d_mesh_out, hbm_d_grid_out,
        mesh_out, grid_out, d_grid_in, res0, res1, res2, res3, res4,
        grid_in, mesh_static, edge_static, send_rows, edge_src, edge_dst, w_grid_in, w_mesh_in, w_edge_in, w_edge_up, w_mesh_up, w_grid_up, w_second, vectors, d_mesh_out, d_grid_out, in_sem,
        grid_lat, mesh_lat, edge_lat, outgoing, incoming, d_incoming, d_outgoing,
        oh_src, oht_src, oh_dst, oht_dst,
        hid0, hid1, hid2, hid3, hid4, hid5,
        ds0, ds1, ds2, ds3, nm0, nm1, nm2, nm3, iv0, iv1, iv2, iv3,
        part3, edge_new, agg, d_grid_lat, d_mesh_lat, d_agg, d_slot, d_node,
        dl_g, dp_g, dl_m, dp_m, dl_e, dp_e,
        par0, par1, par2, par3, par4, ra0, ra1, ra2, ra3, ra4, cs0, cs1, cs2, cs3, cs4, rb0, rb1, rb2, rb3, rb4,
        f_send, f_recv, b_send, b_recv, s0_send, s0_recv, s1_send, s1_recv, s2_send, s2_recv, s3_send, s3_recv, s4_send, s4_recv):
    me = lax.axis_index(AXIS_NAME)
    core = me % 2
    chip = me // 2
    n_grid = grid_lat.shape[0]
    n_mesh = mesh_lat.shape[0]
    n_edge = edge_lat.shape[0]
    slots = send_rows.shape[1]
    pars, ras, css = (par0, par1, par2, par3, par4), (ra0, ra1, ra2, ra3, ra4), (cs0, cs1, cs2, cs3, cs4)
    rbs, ress = (rb0, rb1, rb2, rb3, rb4), (res0, res1, res2, res3, res4)

    def flip(idx, j):
        out = 0
        for b in range(4):
            bit = (idx // (1 << b)) % 2
            out = out + (1 << b) * (1 - bit if (j >> b) & 1 else bit)
        return out

    def loop(name, lo, hi, body, init):
        with jax.named_scope(name):
            return lax.fori_loop(lo, hi, body, init)

    barrier = pltpu.get_barrier_semaphore()
    for j in range(1, N_DEV):
        pl.semaphore_signal(barrier, inc=1, device_id=(flip(me, j),), device_id_type=pl.DeviceIdType.MESH)

    order = ('send_rows', 'grid_in', 'w_grid_in', 'vectors', 'w_second', 'w_grid_up', 'd_grid_out', 'mesh_static', 'w_mesh_in', 'edge_src',
             'edge_dst', 'edge_static', 'w_edge_in', 'w_edge_up', 'w_mesh_up', 'd_mesh_out')
    loads = {
        'grid_in': (hbm_grid_in, grid_in),
        'mesh_static': (hbm_mesh_static, mesh_static),
        'edge_static': (hbm_edge_static, edge_static),
        'send_rows': (hbm_send_rows, send_rows),
        'edge_src': (hbm_edge_src, edge_src),
        'edge_dst': (hbm_edge_dst, edge_dst),
        'w_grid_in': (hbm_w_grid_in, w_grid_in),
        'w_mesh_in': (hbm_w_mesh_in, w_mesh_in),
        'w_edge_in': (hbm_w_edge_in, w_edge_in),
        'w_edge_up': (hbm_w_edge_up, w_edge_up),
        'w_mesh_up': (hbm_w_mesh_up, w_mesh_up),
        'w_grid_up': (hbm_w_grid_up, w_grid_up),
        'w_second': (hbm_w_second, w_second),
        'vectors': (hbm_vectors, vectors),
        'd_mesh_out': (hbm_d_mesh_out, d_mesh_out),
        'd_grid_out': (hbm_d_grid_out, d_grid_out),
    }
    for i, name in enumerate(order):
        loads[name] = pltpu.make_async_copy(loads[name][0], loads[name][1], in_sem.at[i])
        loads[name].start()

    def need(*which):
        for name in which:
            loads[name].wait()

    pending = []

    def send(src, dst, send_sem, recv_sem, dev):
        copy = pltpu.make_async_remote_copy(src_ref=src, dst_ref=dst, send_sem=send_sem, recv_sem=recv_sem,
                                            device_id=(dev,), device_id_type=pl.DeviceIdType.MESH)
        copy.start()

    def settle(ref, sem):
        pltpu.make_async_copy(ref, ref, sem).wait()

    far, near = (15, 14, 11, 10, 13, 12, 9, 8), (7, 6, 3, 2, 5, 4, 1)
    z_bit = me // 8
    chip_order = (7, 3, 5, 6, 1, 2, 4)

    def exchange(src, dst, send_sem, recv_sem, peers):
        for j in peers:
            peer = flip(me, j)
            send(src.at[pl.ds(pl.multiple_of(peer * slots, slots), slots)],
                 dst.at[pl.ds(pl.multiple_of(me * slots, slots), slots)], send_sem, recv_sem, peer)
        if peers is near:
            mine = pl.ds(pl.multiple_of(me * slots, slots), slots)
            dst[mine, :] = src[mine, :]
            pending.append((src.at[pl.ds(0, (N_DEV - 1) * slots)], send_sem))

    def stage0(g):
        half = GROUP_ROWS[g] // 2
        other = pl.ds(pl.multiple_of((1 - core) * half, half), half)
        send(pars[g].at[other], ras[g], s0_send.at[g], s0_recv.at[g], flip(me, 1))
        pending.append((ras[g], s0_send.at[g]))

    def stage1(g):
        with jax.named_scope('s1_%d' % g):
            settle(ras[g], s0_recv.at[g])
            half = GROUP_ROWS[g] // 2
            part = half // N_CHIP
            mine = pl.ds(pl.multiple_of(core * half, half), half)
            total = pars[g][mine, :] + ras[g][...]
            ras[g][...] = total
            css[g][...] = total.astype(BF16)
            for j in chip_order:
                peer = flip(me, 2 * j)
                send(css[g].at[pl.ds(pl.multiple_of((peer // 2) * part, part), part)], rbs[g].at[j - 1],
                     s1_send.at[g], s1_recv.at[g], peer)
            pending.append((rbs[g], s1_send.at[g]))

    def stage2(g):
        with jax.named_scope('s2_%d' % g):
            half = GROUP_ROWS[g] // 2
            part = half // N_CHIP
            settle(rbs[g], s1_recv.at[g])
            total = ras[g][pl.ds(pl.multiple_of(chip * part, part), part), :]
            for j in range(1, N_CHIP):
                total = total + rbs[g][j - 1].astype(F32)
            mine = pl.ds(pl.multiple_of(core * half + chip * part, part), part)
            ress[g][mine, :] = total.astype(BF16)
            peers = (7, 1, 2, 4) if g in RELAYED else chip_order
            for j in peers:
                send(ress[g].at[mine], ress[g].at[mine], s2_send.at[g], s2_recv.at[g], flip(me, 2 * j))
            pending.append((rbs[g].at[pl.ds(0, len(peers))], s2_send.at[g]))

    def relay(g):
        with jax.named_scope('re_%d' % g):
            half = GROUP_ROWS[g] // 2
            part = half // N_CHIP
            settle(rbs[g].at[pl.ds(0, 4)], s2_recv.at[g])
            for origin, target in ((2, 1), (4, 2), (1, 4)):
                rows = pl.ds(pl.multiple_of(core * half + (flip(me, 2 * origin) // 2) * part, part), part)
                send(ress[g].at[rows], ress[g].at[rows], s4_send.at[g], s4_recv.at[g], flip(me, 2 * target))
            pending.append((rbs[g].at[pl.ds(0, 3)], s4_send.at[g]))

    def stage3(g):
        with jax.named_scope('s3_%d' % g):
            half = GROUP_ROWS[g] // 2
            if g in RELAYED:
                settle(rbs[g].at[pl.ds(0, 3)], s4_recv.at[g])
            else:
                settle(rbs[g], s2_recv.at[g])
            mine = pl.ds(pl.multiple_of(core * half, half), half)
            send(ress[g].at[mine], ress[g].at[mine], s3_send.at[g], s3_recv.at[g], flip(me, 1))
            pending.append((css[g], s3_send.at[g]))

    def stage4(g):
        with jax.named_scope('s4_%d' % g):
            settle(css[g], s3_recv.at[g])

    def blk(i, size):
        return pl.ds(pl.multiple_of(i * size, size), size)

    def vec(k, i):
        return vectors[k, i:i + 1, :]

    def mlp_fwd(k, pre):
        x = pre + vec(k, 0)
        sig = jax.nn.sigmoid(x)
        act = x * sig
        hid = act.astype(BF16)
        o = mm(hid, w_second[k]) + vec(k, 1)
        cen = o - jnp.mean(o, axis=-1, keepdims=True)
        inv = lax.rsqrt(jnp.mean(cen * cen, axis=-1, keepdims=True) + LN_EPS)
        nrm = cen * inv
        out = nrm * vec(k, 2) + vec(k, 3)
        dsilu = sig + act * (1.0 - sig)
        return out, hid, dsilu, nrm, inv

    def mlp_bwd(k, dsilu, nrm, inv, d_out):
        dn = d_out * vec(k, 2)
        m1 = jnp.mean(dn, axis=-1, keepdims=True)
        m2 = jnp.mean(dn * nrm, axis=-1, keepdims=True)
        d_lin = inv * (dn - m1 - nrm * m2)
        d_lin_bf = d_lin.astype(BF16)
        d_pre = mm_nt(d_lin_bf, w_second[k]) * dsilu
        return d_lin_bf, d_pre.astype(BF16), (fold8(d_pre), fold8(d_lin), fold8(d_out * nrm), fold8(d_out))

    zeros4 = tuple(jnp.zeros((8, LAT), F32) for _ in range(4))

    def put_vec(k, sums):
        for i in range(4):
            par4[256 + ROW_VEC + 4 * k + i:256 + ROW_VEC + 4 * k + i + 1, :] = jnp.sum(sums[i], axis=0, keepdims=True)

    def add4(a, b):
        return tuple(x + y for x, y in zip(a, b))

    par4[256:512, :] = jnp.zeros((256, LAT), F32)

    need('grid_in', 'w_grid_in', 'vectors', 'w_second')

    def grid_embed(i, c):
        rows = blk(i, BLK_G)
        out, hid, dsilu, nrm, inv = mlp_fwd(0, mm_tn(grid_in[:, rows], w_grid_in[...]))
        grid_lat[rows, :] = out.astype(BF16)
        hid0[rows, :] = hid
        ds0[rows, :] = dsilu
        nm0[rows, :] = nrm
        iv0[rows, :] = inv
        return c

    loop('grid_embed', 0, n_grid // BLK_G, grid_embed, 0)

    def row_pair(i):
        return jnp.concatenate([send_rows[pl.ds(2 * i, 1), :], send_rows[pl.ds(2 * i + 1, 1), :]], axis=1)

    def columns_of(row):
        return jnp.transpose(jnp.broadcast_to(row, (128, 128)))

    def one_hot(col, n):
        lane = lax.broadcasted_iota(jnp.int32, (128, 128), 1).astype(jnp.int16)
        col = col.astype(jnp.int16)
        return jnp.concatenate([jnp.where(col == lane + jnp.full((), 128 * t, jnp.int16), jnp.ones((), BF16), jnp.zeros((), BF16)) for t in range(n // 128)], axis=1)

    def one_hot_t(row, n):
        sub = lax.broadcasted_iota(jnp.int32, (n, 128), 0).astype(jnp.int16)
        return jnp.where(sub == jnp.broadcast_to(row, (n, 128)).astype(jnp.int16), jnp.ones((), BF16), jnp.zeros((), BF16))

    need('send_rows')
    def gather_half(half):
        for t in range(N_DEV // 4):
            i = half * (N_DEV // 4) + t
            pick = one_hot(columns_of(row_pair(i)), n_grid)
            outgoing[blk(i, 128), :] = mm(pick, grid_lat[...]).astype(BF16)

    gather_half(1 - z_bit)
    with jax.named_scope('w_bar'):
        pl.semaphore_wait(barrier, N_DEV - 1)
    exchange(outgoing, incoming, f_send, f_recv, far)
    gather_half(z_bit)
    exchange(outgoing, incoming, f_send, f_recv, near)

    need('w_grid_up', 'd_grid_out')

    def grid_update(i, sums):
        rows = blk(i, BLK_G)
        lat = grid_lat[rows, :]
        out, hid, dsilu, nrm, inv = mlp_fwd(5, mm(lat, w_grid_up[...]))
        grid_out[rows, :] = (lat.astype(F32) + out).astype(BF16)
        d_out = d_grid_out[rows, :].astype(F32)
        d_lin, d_pre, add = mlp_bwd(5, dsilu, nrm, inv, d_out)
        hid5[rows, :] = hid
        dl_g[rows, :] = d_lin
        dp_g[rows, :] = d_pre
        d_grid_lat[rows, :] = d_out + mm_nt(d_pre, w_grid_up[...])
        return add4(sums, add)

    put_vec(5, loop('grid_update', 0, n_grid // BLK_G, grid_update, zeros4))
    par0[0:256, :] = mm_tn(grid_lat[...], dp_g[...])
    par0[256:512, :] = mm_tn(hid5[...], dl_g[...])
    stage0(0)

    need('mesh_static', 'w_mesh_in', 'edge_src', 'edge_dst', 'edge_static', 'w_edge_in', 'w_edge_up')

    def mesh_embed(i, c):
        rows = blk(i, BLK_M)
        out, hid, dsilu, nrm, inv = mlp_fwd(1, mm_tn(mesh_static[:, rows], w_mesh_in[...]))
        mesh_lat[rows, :] = out.astype(BF16)
        hid1[rows, :] = hid
        ds1[rows, :] = dsilu
        nm1[rows, :] = nrm
        iv1[rows, :] = inv
        return c

    loop('mesh_embed', 0, n_mesh // BLK_M, mesh_embed, 0)

    def hots(i, c):
        rows = blk(i, 128)
        src = edge_src[pl.ds(i, 1), :]
        dst = edge_dst[pl.ds(i, 1), :]
        oh_src[rows, :] = one_hot(columns_of(src), n_grid)
        oh_dst[rows, :] = one_hot(columns_of(dst), n_mesh)
        oht_src[:, rows] = one_hot_t(src, n_grid)
        oht_dst[:, rows] = one_hot_t(dst, n_mesh)
        return c

    loop('hots', 0, n_edge // 128, hots, 0)
    stage1(0)

    def edge_embed(i, c):
        rows = blk(i, BLK_E)
        out, hid, dsilu, nrm, inv = mlp_fwd(2, mm_tn(edge_static[:, rows], w_edge_in[...]))
        lat = out.astype(BF16)
        edge_lat[rows, :] = lat
        hid2[rows, :] = hid
        ds2[rows, :] = dsilu
        nm2[rows, :] = nrm
        iv2[rows, :] = inv
        recv = mm(oh_dst[rows, :], mesh_lat[...]).astype(BF16)
        part3[rows, :] = mm(lat, w_edge_up[0:LAT, :]) + mm(recv, w_edge_up[2 * LAT:3 * LAT, :])
        return c

    loop('edge_embed', 0, n_edge // BLK_E, edge_embed, 0)

    with jax.named_scope('w_fwd'):
        settle(incoming.at[pl.ds(0, (N_DEV - 1) * slots)], f_recv)

    def edge_update(i, c):
        rows = blk(i, BLK_E)
        sender = mm(oh_src[rows, :], incoming[...]).astype(BF16)
        out, hid, dsilu, nrm, inv = mlp_fwd(3, part3[rows, :] + mm(sender, w_edge_up[LAT:2 * LAT, :]))
        edge_new[rows, :] = (edge_lat[rows, :].astype(F32) + out).astype(BF16)
        hid3[rows, :] = hid
        ds3[rows, :] = dsilu
        nm3[rows, :] = nrm
        iv3[rows, :] = inv
        return c

    loop('edge_update', 0, n_edge // BLK_E, edge_update, 0)
    stage2(0)

    need('w_mesh_up', 'd_mesh_out')

    def mesh_update(i, sums):
        rows = blk(i, BLK_M)
        total = mm(oht_dst[rows, :], edge_new[...]).astype(BF16)
        agg[rows, :] = total
        lat = mesh_lat[rows, :]
        out, hid, dsilu, nrm, inv = mlp_fwd(4, mm(lat, w_mesh_up[0:LAT, :]) + mm(total, w_mesh_up[LAT:2 * LAT, :]))
        mesh_out[rows, :] = (lat.astype(F32) + out).astype(BF16)
        d_out = d_mesh_out[rows, :].astype(F32)
        d_lin, d_pre, add = mlp_bwd(4, dsilu, nrm, inv, d_out)
        hid4[rows, :] = hid
        dl_m[rows, :] = d_lin
        dp_m[rows, :] = d_pre
        d_mesh_lat[rows, :] = d_out + mm_nt(d_pre, w_mesh_up[0:LAT, :])
        d_agg[rows, :] = mm_nt(d_pre, w_mesh_up[LAT:2 * LAT, :]).astype(BF16)
        return add4(sums, add)

    put_vec(4, loop('mesh_update', 0, n_mesh // BLK_M, mesh_update, zeros4))
    par1[0:256, :] = mm_tn(mesh_lat[...], dp_m[...])
    par1[256:512, :] = mm_tn(agg[...], dp_m[...])
    par1[512:768, :] = mm_tn(hid4[...], dl_m[...])
    stage0(1)

    def edge_back(i, sums):
        rows = blk(i, BLK_E)
        d_out = mm(oh_dst[rows, :], d_agg[...])
        d_lin, d_pre, add = mlp_bwd(3, ds3[rows, :], nm3[rows, :], iv3[rows, :], d_out)
        dl_e[rows, :] = d_lin
        dp_e[rows, :] = d_pre
        part3[rows, :] = d_out + mm_nt(d_pre, w_edge_up[0:LAT, :])
        return add4(sums, add)

    put_vec(3, loop('edge_back', 0, n_edge // BLK_E, edge_back, zeros4))
    stage1(1)

    def slot_back(i, c):
        rows = blk(i, BLK_S)
        d_sum = mm(oht_src[rows, :], dp_e[...]).astype(BF16)
        d_slot[rows, :] = d_sum
        d_incoming[rows, :] = mm_nt(d_sum, w_edge_up[LAT:2 * LAT, :]).astype(BF16)
        return c

    with jax.named_scope('slot_back'):
        slot_back(1 - z_bit, 0)
    exchange(d_incoming, d_outgoing, b_send, b_recv, far)
    with jax.named_scope('slot_back'):
        slot_back(z_bit, 0)
    exchange(d_incoming, d_outgoing, b_send, b_recv, near)

    def node_back(i, c):
        rows = blk(i, BLK_M)
        d_sum = mm(oht_dst[rows, :], dp_e[...]).astype(BF16)
        d_node[rows, :] = d_sum
        d_mesh_lat[rows, :] = d_mesh_lat[rows, :] + mm_nt(d_sum, w_edge_up[2 * LAT:3 * LAT, :])
        return c

    loop('node_back', 0, n_mesh // BLK_M, node_back, 0)
    par2[0:256, :] = mm_tn(edge_lat[...], dp_e[...])
    par2[256:512, :] = mm_tn(incoming[...], d_slot[...])
    par2[512:768, :] = mm_tn(mesh_lat[...], d_node[...])
    par2[768:1024, :] = mm_tn(hid3[...], dl_e[...])
    stage0(2)

    def mesh_in_back(i, sums):
        rows = blk(i, BLK_M)
        d_lin, d_pre, add = mlp_bwd(1, ds1[rows, :], nm1[rows, :], iv1[rows, :], d_mesh_lat[rows, :])
        dl_m[rows, :] = d_lin
        dp_m[rows, :] = d_pre
        return add4(sums, add)

    put_vec(1, loop('mesh_in_back', 0, n_mesh // BLK_M, mesh_in_back, zeros4))
    def edge_in_back(i, sums):
        rows = blk(i, BLK_E)
        d_lin, d_pre, add = mlp_bwd(2, ds2[rows, :], nm2[rows, :], iv2[rows, :], part3[rows, :])
        dl_e[rows, :] = d_lin
        dp_e[rows, :] = d_pre
        return add4(sums, add)

    put_vec(2, loop('edge_in_back', 0, n_edge // BLK_E, edge_in_back, zeros4))
    par3[0:256, :] = mm_tn(hid2[...], dl_e[...])
    par3[256:512, :] = mm_tn(hid1[...], dl_m[...])
    stage0(3)
    stage1(2)
    stage2(1)
    stage3(0)
    par4[256 + ROW_EDGE_IN:256 + ROW_EDGE_IN + 4, :] = mm(edge_static[...], dp_e[...])
    par4[256 + ROW_MESH_IN:256 + ROW_MESH_IN + 3, :] = mm(mesh_static[...], dp_m[...])
    stage1(3)

    with jax.named_scope('w_bwd'):
        settle(d_outgoing.at[pl.ds(0, (N_DEV - 1) * slots)], b_recv)

    all_rows = jnp.concatenate([row_pair(i) for i in range(N_DEV // 2)], axis=1)

    def grid_in_back(i, sums):
        rows = blk(i, BLK_G)
        sub = lax.broadcasted_iota(jnp.int32, (BLK_G, N_DEV * slots), 0) + i * BLK_G
        spread = jnp.where(sub == all_rows, 1.0, 0.0).astype(BF16)
        d_out = d_grid_lat[rows, :] + mm(spread, d_outgoing[...])
        d_lin, d_pre, add = mlp_bwd(0, ds0[rows, :], nm0[rows, :], iv0[rows, :], d_out)
        dl_g[rows, :] = d_lin
        dp_g[rows, :] = d_pre
        d_grid_in[:, rows] = mm_nt(w_grid_in[...], d_pre)
        return add4(sums, add)

    put_vec(0, loop('grid_in_back', 0, n_grid // BLK_G, grid_in_back, zeros4))
    with jax.named_scope("dw0"):
        par4[0:256, :] = mm_tn(hid0[...], dl_g[...])
        par4[256:256 + grid_in.shape[0], :] = mm(grid_in[...], dp_g[...])
        stage0(4)
    relay(1)
    stage1(4)
    stage2(2)
    stage2(3)
    stage3(1)
    relay(2)
    stage2(4)
    relay(3)
    stage3(2)
    stage3(3)
    stage3(4)
    for g in range(N_GROUP):
        stage4(g)
    with jax.named_scope("t_send"):
        for ref, sem in pending:
            settle(ref, sem)


def final_kernel(mesh_res, grid_res, d_grid_res, res0, res1, res2, res3, res4,
                 mesh_out, grid_out, d_grid_in, d_w_grid_in, d_w_mesh_in, d_w_edge_in, d_w_edge_up, d_w_mesh_up, d_w_grid_up, d_w_second, d_vectors,
                 b_grid_in, b_mesh_in, b_edge_in, b_edge_up, b_mesh_up, b_grid_up, b_second, b_vectors, sems):
    plan = []
    started = []

    def start(src, dst):
        copy = pltpu.make_async_copy(src, dst, sems.at[len(started)])
        copy.start()
        started.append(copy)

    def put(src, rows, buf, dst):
        buf[...] = src[rows[0]:rows[1], :].astype(F32)
        plan.append((buf, dst))
        if len(plan) > 1:
            start(*plan[-2])

    start(d_grid_res, d_grid_in)
    start(grid_res, grid_out)
    start(mesh_res, mesh_out)
    put(res2, (0, 768), b_edge_up, d_w_edge_up)
    put(res1, (0, 512), b_mesh_up, d_w_mesh_up)
    put(res0, (0, 256), b_grid_up, d_w_grid_up)
    put(res0, (256, 512), b_second.at[5], d_w_second.at[5])
    put(res1, (512, 768), b_second.at[4], d_w_second.at[4])
    put(res2, (768, 1024), b_second.at[3], d_w_second.at[3])
    put(res3, (0, 256), b_second.at[2], d_w_second.at[2])
    put(res3, (256, 512), b_second.at[1], d_w_second.at[1])
    put(res4, (0, 256), b_second.at[0], d_w_second.at[0])
    small = res4[256:512, :].astype(F32)
    b_edge_in[...] = small[ROW_EDGE_IN:ROW_EDGE_IN + 4, :]
    b_mesh_in[...] = small[ROW_MESH_IN:ROW_MESH_IN + 3, :]
    b_vectors[...] = small[ROW_VEC:ROW_VEC + 24, :].reshape(6, 4, LAT)
    b_grid_in[...] = small[0:b_grid_in.shape[0], :]
    start(*plan[-1])
    start(b_edge_in, d_w_edge_in)
    start(b_mesh_in, d_w_mesh_in)
    start(b_vectors, d_vectors)
    start(b_grid_in, d_w_grid_in)
    for copy in started:
        copy.wait()


def solution(mesh):
    row_spec = P(AXIS_NAME, None)
    edge_spec = P(AXIS_NAME)
    rep_spec = P()
    in_specs = (row_spec, row_spec, row_spec, row_spec, edge_spec, edge_spec) + (rep_spec,) * 8 + (row_spec, row_spec)
    out_specs = (row_spec, row_spec, row_spec) + (rep_spec,) * 8

    def local_step(grid_in, mesh_static, edge_static, send_rows, edge_src, edge_dst, *rest):
        n_grid, feats = grid_in.shape
        n_mesh = mesh_static.shape[0]
        n_edge = edge_static.shape[0]
        n_slot = send_rows.size
        src2 = edge_src.reshape(n_edge // 128, 128)
        dst2 = edge_dst.reshape(n_edge // 128, 128)

        def vm(shape, dtype):
            return pltpu.VMEM(shape, dtype)

        def rows_bf(n):
            return vm((n, LAT), BF16)

        def rows_f32(n):
            return vm((n, LAT), F32)

        dma = pltpu.SemaphoreType.DMA
        args = (grid_in.T, mesh_static.T, edge_static.T, send_rows, src2, dst2) + rest
        scratch = [vm(a.shape, a.dtype) for a in args] + [dma((len(args),))]
        scratch += [
            rows_bf(n_grid), rows_bf(n_mesh), rows_bf(n_edge), rows_bf(n_slot), rows_bf(n_slot), rows_bf(n_slot), rows_bf(n_slot),
            vm((n_edge, n_slot), BF16), vm((n_slot, n_edge), BF16), vm((n_edge, n_mesh), BF16), vm((n_mesh, n_edge), BF16),
            rows_bf(n_grid), rows_bf(n_mesh), rows_bf(n_edge), rows_bf(n_edge), rows_bf(n_mesh), rows_bf(n_grid),
            rows_f32(n_grid), rows_f32(n_mesh), rows_f32(n_edge), rows_f32(n_edge),
            rows_f32(n_grid), rows_f32(n_mesh), rows_f32(n_edge), rows_f32(n_edge),
            vm((n_grid, 1), F32), vm((n_mesh, 1), F32), vm((n_edge, 1), F32), vm((n_edge, 1), F32),
            rows_f32(n_edge), rows_bf(n_edge), rows_bf(n_mesh), rows_f32(n_grid), rows_f32(n_mesh), rows_bf(n_mesh), rows_bf(n_slot), rows_bf(n_mesh),
            rows_bf(n_grid), rows_bf(n_grid), rows_bf(n_mesh), rows_bf(n_mesh), rows_bf(n_edge), rows_bf(n_edge),
        ]
        scratch += [rows_f32(r) for r in GROUP_ROWS]
        scratch += [rows_f32(r // 2) for r in GROUP_ROWS]
        scratch += [rows_bf(r // 2) for r in GROUP_ROWS]
        scratch += [vm((7, r // 16, LAT), BF16) for r in GROUP_ROWS]
        scratch += [dma] * 4 + [dma((N_GROUP,))] * 10
        shape = jax.ShapeDtypeStruct
        outs = (shape((n_mesh, LAT), BF16), shape((n_grid, LAT), BF16), shape((feats, n_grid), F32)) + tuple(shape((r, LAT), BF16) for r in GROUP_ROWS)
        vspec = pl.BlockSpec(memory_space=pltpu.VMEM)
        results = pl.pallas_call(
            main_kernel,
            out_shape=tuple(pltpu.VMEM(o.shape, o.dtype) for o in outs),
            in_specs=[pl.BlockSpec(memory_space=pltpu.MemorySpace.HBM)] * 16,
            out_specs=tuple([vspec] * len(outs)),
            scratch_shapes=scratch,
            compiler_params=pltpu.CompilerParams(collective_id=0, has_side_effects=True, vmem_limit_bytes=62300 * 1024),
        )(*args)

        finals = (shape((n_mesh, LAT), BF16), shape((n_grid, LAT), BF16), shape((feats, n_grid), F32),
                  shape((feats, LAT), F32), shape((3, LAT), F32), shape((4, LAT), F32), shape((3 * LAT, LAT), F32),
                  shape((2 * LAT, LAT), F32), shape((LAT, LAT), F32), shape((6, LAT, LAT), F32), shape((6, 4, LAT), F32))
        done = pl.pallas_call(
            final_kernel,
            out_shape=finals,
            in_specs=[vspec] * len(outs),
            out_specs=tuple([pl.BlockSpec(memory_space=pltpu.MemorySpace.HBM)] * len(finals)),
            scratch_shapes=[vm(f.shape, f.dtype) for f in finals[3:]] + [dma((16,))],
            compiler_params=pltpu.CompilerParams(vmem_limit_bytes=16 * 1024 * 1024),
        )(*results)
        return done[:2] + (done[2].T,) + done[3:]

    return jax.shard_map(local_step, mesh=mesh, in_specs=in_specs, out_specs=out_specs, check_vma=False)
```
